128 devices in a mesh: lat: 2 (over x_lo), lon: 8 (over z_lo, x_hi, core), lev: 8 (over z_hi, y).
Axes of the slice: x: 4 (x_hi: 2, x_lo: 2; x = x_hi * 2 + x_lo), y: 4, z: 4 (z_hi: 2, z_lo: 2; z = z_hi * 2 + z_lo), core: 2. Of those that a mesh axis runs over, the one named last changes fastest.
Arguments:
- initial_state: float32 [16, 256, 512, 128], P('lat', 'lon', 'lev'), may hold values from 0.2 to 1.8
- scaled_diffusivity: float32 [16, 256, 512, 128], P('lat', 'lon', 'lev'), may hold values from 0.03 to 0.15
- scaled_forcing: float32 [16, 256, 512, 128], P('lat', 'lon', 'lev'), may hold values from -0.2 to 0.2
Outputs:
- cumulative_totals: float32 [16, 256, 512, 128], P('lat', 'lon', 'lev')
- temperature_end: float32 [16, 256, 512, 128], P('lat', 'lon', 'lev')
The draws below stay inside these ranges and needn't reach their ends.
All inputs are finite; a program needn't handle non-finite values.
Results may differ from the reference program's by a relative error of at most 0.00002.
Values sent between devices are 32-bit elements; how exact they have to be, the bound alone decides.
A program may use at most 128 MiB of HBM per device.

```python
import jax
import jax.numpy as jnp
from jax import lax

SECOND_EXTENT = 16
FIRST_EXTENT = 256
THIRD_EXTENT = 512
MEMBER_TALLY = 128
STEPS = 4


def level_of(rng, extent, cuts, smallest, top_value):
    def one(axis_at, shards_of):
        draws = jax.random.uniform(jax.random.fold_in(jax.random.fold_in(rng, 6), axis_at), (shards_of,), jnp.float32, smallest / len(cuts), top_value / len(cuts))
        return jnp.repeat(jnp.exp(draws), extent[axis_at] // shards_of).reshape((-1,) + (1,) * (len(extent) - axis_at - 1))

    level = one(*cuts[0])
    for cut in cuts[1:]:
        level = level * one(*cut)
    return level


def setup_inputs(seed: int = 0) -> dict:
    seeds = jax.random.split(jax.random.key(seed), 4)
    initial_state = jnp.clip(0.2 + 1.5999999 * jax.random.uniform(seeds[0], (SECOND_EXTENT, FIRST_EXTENT, THIRD_EXTENT, MEMBER_TALLY), jnp.float32) ** level_of(seeds[0], (SECOND_EXTENT, FIRST_EXTENT, THIRD_EXTENT, MEMBER_TALLY), ((0, 2), (1, 8), (2, 8)), -0.2, 0.2), 0.2, 1.8)
    scaled_diffusivity = jnp.clip(0.03 + 0.120000007 * jax.random.uniform(seeds[1], (SECOND_EXTENT, FIRST_EXTENT, THIRD_EXTENT, MEMBER_TALLY), jnp.float32) ** level_of(seeds[1], (SECOND_EXTENT, FIRST_EXTENT, THIRD_EXTENT, MEMBER_TALLY), ((0, 2), (1, 8), (2, 8)), -0.2, 0.2), 0.03, 0.15)
    scaled_forcing = jnp.clip(jax.random.uniform(seeds[2], (SECOND_EXTENT, FIRST_EXTENT, THIRD_EXTENT, MEMBER_TALLY), jnp.float32, -0.2, 0.2) * level_of(seeds[2], (SECOND_EXTENT, FIRST_EXTENT, THIRD_EXTENT, MEMBER_TALLY), ((0, 2), (1, 8), (2, 8)), -0.4, 0.0), -0.2, 0.2)
    return dict(initial_state=initial_state, scaled_diffusivity=scaled_diffusivity, scaled_forcing=scaled_forcing)


def strip_edges(values, dims):
    for dim in dims:
        values = lax.slice_in_dim(values, 1, values.shape[dim] - 1, axis=dim)
    return values


def neighbour(values, dim, start, dims):
    others = [other for other in dims if other != dim]
    values = strip_edges(values, others)
    return lax.slice_in_dim(values, start, start + values.shape[dim] - 2, axis=dim)


def explicit_update(haloed_values, scaled_diffusivity, scaled_forcing):
    middle = strip_edges(haloed_values, (0, 1, 2))
    lower = [neighbour(haloed_values, dim, 0, (0, 1, 2)) for dim in (0, 1, 2)]
    upper = [neighbour(haloed_values, dim, 2, (0, 1, 2)) for dim in (0, 1, 2)]
    spread = lower[0] + upper[0] + lower[1] + upper[1] + lower[2] + upper[2] - 6.0 * middle
    return middle + scaled_diffusivity * spread + scaled_forcing


def reference(initial_state, scaled_diffusivity, scaled_forcing):
    for step in range(STEPS):
        initial_state = explicit_update(jnp.pad(initial_state, ((1, 1), (1, 1), (1, 1), (0, 0)), mode="constant"), scaled_diffusivity, scaled_forcing)
    cumulative_totals = jnp.cumsum(initial_state, axis=1) / FIRST_EXTENT
    return cumulative_totals, initial_state
```

```python
import functools

import jax
import jax.numpy as jnp
from jax import lax
from jax.experimental import pallas as pl
from jax.experimental.pallas import tpu as pltpu
from jax.sharding import PartitionSpec as P

STEPS = 4
PAD = 8
CHUNK = 8
CORES = 2
MESH = pl.DeviceIdType.MESH


def steps_kernel(
    sizes, x, d, f, end, before, even, odd, coef, source,
    lev_out, lev_in, total, mate, chip, chip_in,
    lat_send, lat_recv, lon_send, lon_recv, lev_send, lev_recv,
    load_sem, mate_send, mate_recv, chip_send, chip_recv,
):
    J, I, K, M = x.shape
    chunks = K // CHUNK
    states = (even, odd)
    me = {axis: lax.axis_index(axis) for axis in sizes}
    n_lon = sizes["lon"]
    n_chips = n_lon // CORES
    my_chip = me["lon"] // CORES
    my_core = me["lon"] % CORES
    rows = pl.ds(1, I)
    levels = pl.ds(PAD, K)
    planes = pl.ds(1, J)

    def has(axis, side):
        return me[axis] > 0 if side == 0 else me[axis] < sizes[axis] - 1

    def beside(axis, side):
        return {axis: me[axis] - 1 if side == 0 else me[axis] + 1}

    def both(axis, act):
        if sizes[axis] > 1:
            for side in (0, 1):
                pl.when(has(axis, side))(functools.partial(act, side))

    def load(which, j):
        src, dst = (
            (x.at[j], even.at[j + 1, rows, levels]),
            (d.at[j], coef.at[j]),
            (f.at[j], source.at[j]),
        )[which]
        return pltpu.make_async_copy(src, dst, load_sem.at[which, j])

    for which in range(3):
        for j in range(J):
            load(which, j).start()

    barrier = pltpu.get_barrier_semaphore()
    count = jnp.int32(n_lon - 1)

    def greet(target):
        pl.semaphore_signal(barrier, inc=1, device_id=target, device_id_type=MESH)

    for axis in ("lat", "lev"):
        both(axis, lambda side, axis=axis: greet(beside(axis, side)))
        if sizes[axis] > 1:
            count = count + has(axis, 0).astype(jnp.int32) + has(axis, 1).astype(jnp.int32)
    for other in range(n_lon):
        pl.when(other != me["lon"])(lambda other=other: greet({"lon": jnp.int32(other)}))
    pl.semaphore_wait(barrier, count)

    def inside(c):
        return pl.ds(pl.multiple_of(c * CHUNK, CHUNK), CHUNK)

    def padded(c):
        return pl.ds(pl.multiple_of(PAD + c * CHUNK, CHUNK), CHUNK)

    def lat_copy(step, side, c, arriving=False):
        slot = step % 2
        state = states[slot]
        plane, target = (1, J + 1) if side == 0 else (J, 0)
        if arriving:
            target = 0 if side == 0 else J + 1
        if step == 0:
            src = x.at[plane - 1, :, inside(c)]
        else:
            src = state.at[plane, rows, padded(c)]
        return pltpu.make_async_remote_copy(
            src_ref=src,
            dst_ref=state.at[target, rows, padded(c)],
            send_sem=lat_send.at[slot, side, c],
            recv_sem=lat_recv.at[slot, side if arriving else 1 - side, c],
            device_id=beside("lat", side),
            device_id_type=MESH,
        )

    def lon_copy(step, side, c, arriving=False):
        slot = step % 2
        state = states[slot]
        row, target = (1, I + 1) if side == 0 else (I, 0)
        if arriving:
            target = 0 if side == 0 else I + 1
        if step == 0:
            src = x.at[:, row - 1, inside(c)]
        else:
            src = state.at[planes, row, padded(c)]
        return pltpu.make_async_remote_copy(
            src_ref=src,
            dst_ref=state.at[planes, target, padded(c)],
            send_sem=lon_send.at[slot, side, c],
            recv_sem=lon_recv.at[slot, side if arriving else 1 - side, c],
            device_id=beside("lon", side),
            device_id_type=MESH,
        )

    def lev_copy(step, side, arriving=False):
        slot = step % 2
        landing = side if arriving else 1 - side
        return pltpu.make_async_remote_copy(
            src_ref=lev_out.at[slot, side],
            dst_ref=lev_in.at[slot, landing],
            send_sem=lev_send.at[slot, side],
            recv_sem=lev_recv.at[slot, landing],
            device_id=beside("lev", side),
            device_id_type=MESH,
        )

    def send_chunk(step, c):
        both("lon", lambda side: lon_copy(step, side, c).start())
        both("lat", lambda side: lat_copy(step, side, c).start())

    def sent_chunk(step, c):
        both("lon", lambda side: lon_copy(step, side, c).wait_send())
        both("lat", lambda side: lat_copy(step, side, c).wait_send())

    def send_lev(step, side):
        state = states[step % 2]
        row = PAD if side == 0 else PAD + K - 1

        @pl.loop(1, J + 1)
        def _(p):
            lev_out[step % 2, side, p - 1] = state[p, 1 : I + 1, row : row + 1, :]

        lev_copy(step, side).start()

    def take_lev(step, side):
        state = states[step % 2]
        row = PAD - 1 if side == 0 else PAD + K
        lev_copy(step, side, True).wait_recv()

        @pl.loop(1, J + 1)
        def _(p):
            state[p, 1 : I + 1, row : row + 1, :] = lev_in[step % 2, side, p - 1]

    @pl.loop(0, chunks)
    def _(c):
        send_chunk(0, c)

    def clear(axis, side):
        for state in states:
            if axis == "lat":
                target = 0 if side == 0 else J + 1

                @pl.loop(1, I + 1)
                def _(i):
                    state[target, i, PAD : PAD + K, :] = jnp.zeros((K, M), jnp.float32)
            elif axis == "lon":
                target = 0 if side == 0 else I + 1
                for p in range(1, J + 1):
                    state[p, target, PAD : PAD + K, :] = jnp.zeros((K, M), jnp.float32)
            else:
                target = PAD - 1 if side == 0 else PAD + K

                @pl.loop(1, J + 1)
                def _(p):
                    state[p, 1 : I + 1, target : target + 1, :] = jnp.zeros(
                        (I, 1, M), jnp.float32
                    )

    for axis in ("lat", "lon", "lev"):
        for side in (0, 1):
            pl.when(jnp.logical_not(has(axis, side)))(functools.partial(clear, axis, side))

    for j in range(J):
        load(0, j).wait()
    both("lev", lambda side: send_lev(0, side))
    for j in range(J):
        load(1, j).wait()
        load(2, j).wait()

    def update(step, c):
        now, later = states[step % 2], states[(step + 1) % 2]
        last = step == STEPS - 1
        start = pl.multiple_of(PAD + c * CHUNK, CHUNK)
        here = pl.ds(start, CHUNK)
        inner = inside(c)

        def row(i, carry):
            past, mid, sums = carry
            coming = tuple(now[p, i + 1, here, :] for p in range(1, J + 1))
            column = (now[0, i, here, :],) + mid + (now[J + 1, i, here, :],)
            out = []
            for p in range(1, J + 1):
                spread = (
                    (column[p - 1] + column[p + 1])
                    + (past[p - 1] + coming[p - 1])
                    + (
                        now[p, i, pl.ds(start - 1, CHUNK), :]
                        + now[p, i, pl.ds(start + 1, CHUNK), :]
                    )
                    - 6.0 * column[p]
                )
                new = (
                    column[p]
                    + coef[p - 1, i - 1, inner, :] * spread
                    + source[p - 1, i - 1, inner, :]
                )
                if last:
                    end[p - 1, i - 1, inner, :] = new
                else:
                    later[p, i, here, :] = new
                out.append(new)
            if last:
                sums = tuple(total + new for total, new in zip(sums, out))
            return mid, coming, sums

        zero = jnp.zeros((CHUNK, M), jnp.float32)
        _, _, sums = lax.fori_loop(
            1,
            I + 1,
            row,
            (
                tuple(now[p, 0, here, :] for p in range(1, J + 1)),
                tuple(now[p, 1, here, :] for p in range(1, J + 1)),
                (zero,) * J if last else (),
            ),
            unroll=2,
        )
        return sums

    def mate_copy(c):
        return pltpu.make_async_remote_copy(
            src_ref=total.at[:, inside(c)],
            dst_ref=mate.at[:, inside(c)],
            send_sem=mate_send.at[c],
            recv_sem=mate_recv.at[c],
            device_id={"lon": me["lon"] + 1 - 2 * my_core},
            device_id_type=MESH,
        )

    def chip_copy(target, c, arriving=None):
        sender = my_chip if arriving is None else arriving
        return pltpu.make_async_remote_copy(
            src_ref=chip.at[:, inside(c)],
            dst_ref=chip_in.at[sender, :, inside(c)],
            send_sem=chip_send.at[target, c],
            recv_sem=chip_recv.at[sender, c],
            device_id={"lon": target * CORES + my_core},
            device_id_type=MESH,
        )

    def later_chips(act):
        for other in range(1, n_chips):
            pl.when(other > my_chip)(functools.partial(act, other))

    def earlier_chips(act):
        for other in range(n_chips - 1):
            pl.when(other < my_chip)(functools.partial(act, other))

    def share(c):
        mate_copy(c).wait()
        chip[:, inside(c), :] = total[:, inside(c), :] + mate[:, inside(c), :]
        later_chips(lambda other: chip_copy(other, c).start())

    for step in range(STEPS):
        last = step == STEPS - 1

        @pl.loop(0, chunks)
        def _(c):
            if step > 0:
                sent_chunk(step - 1, c)
            both("lon", lambda side: lon_copy(step, side, c, True).wait_recv())
            both("lat", lambda side: lat_copy(step, side, c, True).wait_recv())
            for side, edge in ((0, 0), (1, chunks - 1)):
                if sizes["lev"] > 1:
                    pl.when(jnp.logical_and(c == edge, has("lev", side)))(
                        functools.partial(take_lev, step, side)
                    )
            sums = update(step, c)
            if last:
                for p in range(J):
                    total[p, inside(c), :] = sums[p]
                mate_copy(c).start()
                pl.when(c > 0)(lambda: share(c - 1))
            else:
                send_chunk(step + 1, c)
                for side, edge in ((0, 0), (1, chunks - 1)):

                    def pass_on(side=side):
                        if step > 0:
                            lev_copy(step - 1, side).wait_send()
                        send_lev(step + 1, side)

                    if sizes["lev"] > 1:
                        pl.when(jnp.logical_and(c == edge, has("lev", side)))(pass_on)

    share(chunks - 1)
    before[...] = jnp.where(my_core == 1, mate[...], 0.0)

    def add(other):
        for c in range(chunks):
            chip_copy(0, c, other).wait_recv()
        before[...] += chip_in[other]

    earlier_chips(add)

    for step in (STEPS - 2, STEPS - 1):
        both("lev", lambda side: lev_copy(step, side).wait_send())
    for c in range(chunks):
        sent_chunk(STEPS - 1, c)
        later_chips(lambda other: chip_copy(other, c).wait_send())


def totals_kernel(scale, x, before, totals, end, sums, end_sem, sums_sem):
    J, I = x.shape[:2]

    def out(which, j):
        src, dst, sem = ((x, end, end_sem), (sums, totals, sums_sem))[which]
        return pltpu.make_async_copy(src.at[j], dst.at[j], sem.at[j])

    for j in range(J):
        out(0, j).start()

    @pl.loop(0, J)
    def _(j):
        def row(i, total):
            total = total + x[j, i]
            sums[j, i] = total * scale
            return total

        lax.fori_loop(0, I, row, before[j], unroll=4)
        out(1, j).start()

    for j in range(J):
        out(0, j).wait()
        out(1, j).wait()


def per_device(sizes, initial_state, scaled_diffusivity, scaled_forcing):
    J, I, K, M = initial_state.shape
    chunks = K // CHUNK
    n_lon = sizes["lon"]
    n_chips = n_lon // CORES
    f32 = jnp.float32
    vmem = lambda *shape: pltpu.VMEM(shape, f32)
    sem = lambda *shape: pltpu.SemaphoreType.DMA(shape)
    hbm = pl.BlockSpec(memory_space=pltpu.HBM)
    local = pl.BlockSpec(memory_space=pltpu.VMEM)
    end, before = pl.pallas_call(
        functools.partial(steps_kernel, sizes),
        out_shape=(vmem(J, I, K, M), vmem(J, K, M)),
        in_specs=[hbm] * 3,
        out_specs=(local, local),
        scratch_shapes=[
            vmem(J + 2, I + 2, K + 2 * PAD, M),
            vmem(J + 2, I + 2, K + 2 * PAD, M),
            vmem(J, I, K, M),
            vmem(J, I, K, M),
            vmem(2, 2, J, I, 1, M),
            vmem(2, 2, J, I, 1, M),
            vmem(J, K, M),
            vmem(J, K, M),
            vmem(J, K, M),
            vmem(n_chips, J, K, M),
            sem(2, 2, chunks),
            sem(2, 2, chunks),
            sem(2, 2, chunks),
            sem(2, 2, chunks),
            sem(2, 2),
            sem(2, 2),
            sem(3, J),
            sem(chunks),
            sem(chunks),
            sem(n_chips, chunks),
            sem(n_chips, chunks),
        ],
        compiler_params=pltpu.CompilerParams(
            collective_id=0, has_side_effects=True, vmem_limit_bytes=50 * 2**20
        ),
        name="steps",
    )(initial_state, scaled_diffusivity, scaled_forcing)

    return pl.pallas_call(
        functools.partial(totals_kernel, 1.0 / (I * n_lon)),
        out_shape=(jax.ShapeDtypeStruct((J, I, K, M), f32),) * 2,
        in_specs=[local, local],
        out_specs=(hbm, hbm),
        scratch_shapes=[vmem(J, I, K, M), sem(J), sem(J)],
        compiler_params=pltpu.CompilerParams(vmem_limit_bytes=20 * 2**20),
        name="totals",
    )(end, before)


def solution(mesh):
    spec = P("lat", "lon", "lev", None)
    return jax.shard_map(
        functools.partial(per_device, dict(mesh.shape)),
        mesh=mesh,
        in_specs=(spec,) * 3,
        out_specs=(spec,) * 2,
        check_vma=False,
    )
```

```python
import functools

import jax
import jax.numpy as jnp
from jax import lax
from jax.experimental import pallas as pl
from jax.experimental.pallas import tpu as pltpu
from jax.sharding import PartitionSpec as P

STEPS = 4
PAD = 8
CHUNK = 8
CORES = 2
EARLY = 2
RELAYS = 3
MESH = pl.DeviceIdType.MESH


def steps_kernel(
    sizes, x, d, f, end, before, even, odd, coef, source,
    lev_out, lev_in, total, mate, chip, chip_in, mine, theirs, edge, edge_in, relay,
    lat_send, lat_recv, lon_send, lon_recv, lev_send, lev_recv,
    load_sem, mate_send, mate_recv, chip_send, chip_recv, half_sem, edge_send, edge_recv,
    relay_send, relay_recv, pass_send, pass_recv,
):
    J, I, K, M = x.shape
    chunks = K // CHUNK
    states = (even, odd)
    me = {axis: lax.axis_index(axis) for axis in sizes}
    n_lon = sizes["lon"]
    n_chips = n_lon // CORES
    my_chip = me["lon"] // CORES
    my_core = me["lon"] % CORES
    half = J // CORES
    rows = pl.ds(1, I)
    levels = pl.ds(PAD, K)
    planes = pl.ds(1, J)

    def has(axis, side):
        return me[axis] > 0 if side == 0 else me[axis] < sizes[axis] - 1

    def beside(axis, side):
        return {axis: me[axis] - 1 if side == 0 else me[axis] + 1}

    def both(axis, act):
        if sizes[axis] > 1:
            for side in (0, 1):
                pl.when(has(axis, side))(functools.partial(act, side))

    def load(which, j):
        src, dst = (
            (x.at[j], even.at[j + 1, rows, levels]),
            (d.at[j], coef.at[j]),
            (f.at[j], source.at[j]),
        )[which]
        return pltpu.make_async_copy(src, dst, load_sem.at[which, j])

    for which in range(3):
        for j in range(J):
            load(which, j).start()

    barrier = pltpu.get_barrier_semaphore()
    count = jnp.int32(n_lon - 1)

    def greet(target):
        pl.semaphore_signal(barrier, inc=1, device_id=target, device_id_type=MESH)

    for axis in ("lat", "lev"):
        both(axis, lambda side, axis=axis: greet(beside(axis, side)))
        if sizes[axis] > 1:
            count = count + has(axis, 0).astype(jnp.int32) + has(axis, 1).astype(jnp.int32)
    for other in range(n_lon):
        pl.when(other != me["lon"])(lambda other=other: greet({"lon": jnp.int32(other)}))
    pl.semaphore_wait(barrier, count)

    def inside(c):
        return pl.ds(pl.multiple_of(c * CHUNK, CHUNK), CHUNK)

    def padded(c):
        return pl.ds(pl.multiple_of(PAD + c * CHUNK, CHUNK), CHUNK)

    def lat_copy(step, side, c, arriving=False):
        slot = step % 2
        state = states[slot]
        plane, target = (1, J + 1) if side == 0 else (J, 0)
        if arriving:
            target = 0 if side == 0 else J + 1
        if step == 0:
            src = x.at[plane - 1, :, inside(c)]
        else:
            src = state.at[plane, rows, padded(c)]
        return pltpu.make_async_remote_copy(
            src_ref=src,
            dst_ref=state.at[target, rows, padded(c)],
            send_sem=lat_send.at[slot, side, c],
            recv_sem=lat_recv.at[slot, side if arriving else 1 - side, c],
            device_id=beside("lat", side),
            device_id_type=MESH,
        )

    def lon_copy(step, side, c, arriving=False, count=J):
        slot = step % 2
        state = states[slot]
        row, target = (1, I + 1) if side == 0 else (I, 0)
        if arriving:
            target = 0 if side == 0 else I + 1
        if step == 0:
            src = x.at[pl.ds(0, count), row - 1, inside(c)]
        else:
            src = state.at[pl.ds(1, count), row, padded(c)]
        return pltpu.make_async_remote_copy(
            src_ref=src,
            dst_ref=state.at[pl.ds(1, count), target, padded(c)],
            send_sem=lon_send.at[slot, side, c],
            recv_sem=lon_recv.at[slot, side if arriving else 1 - side, c],
            device_id=beside("lon", side),
            device_id_type=MESH,
        )

    def to_relay(step, side, c):
        row = 1 if side == 0 else I
        if step == 0:
            src = x.at[pl.ds(half, half), row - 1, inside(c)]
        else:
            src = states[step % 2].at[pl.ds(1 + half, half), row, padded(c)]
        return pltpu.make_async_remote_copy(
            src_ref=src,
            dst_ref=relay.at[step, :, inside(c)],
            send_sem=relay_send.at[step, c],
            recv_sem=relay_recv.at[step, c],
            device_id={"lon": jnp.int32(0 if side == 0 else n_lon - 1)},
            device_id_type=MESH,
        )

    def from_relay(step, side, c):
        target = I + 1 if side == 0 else 0
        return pltpu.make_async_remote_copy(
            src_ref=relay.at[step, :, inside(c)],
            dst_ref=states[step % 2].at[pl.ds(1 + half, half), target, padded(c)],
            send_sem=pass_send.at[step, c],
            recv_sem=pass_recv.at[step, c],
            device_id={"lon": jnp.int32(n_lon // 2 - 1 if side == 0 else n_lon // 2)},
            device_id_type=MESH,
        )

    def lon_each(step, whole, split):
        for side in (0, 1):
            halved = me["lon"] == (n_lon // 2 if side == 0 else n_lon // 2 - 1)
            if step < RELAYS:
                pl.when(jnp.logical_and(has("lon", side), jnp.logical_not(halved)))(
                    functools.partial(whole, side)
                )
                pl.when(halved)(functools.partial(split, side))
            else:
                pl.when(has("lon", side))(functools.partial(whole, side))

    def start_lon(step, c):
        def split(side):
            to_relay(step, side, c).start()
            lon_copy(step, side, c, count=half).start()

        lon_each(step, lambda side: lon_copy(step, side, c).start(), split)

    def sent_lon(step, c):
        def split(side):
            to_relay(step, side, c).wait_send()
            lon_copy(step, side, c, count=half).wait_send()

        lon_each(step, lambda side: lon_copy(step, side, c).wait_send(), split)

    def arrived_lon(step, c):
        def split(side):
            from_relay(step, 1 - side, c).wait_recv()
            lon_copy(step, side, c, True, half).wait_recv()

        lon_each(step, lambda side: lon_copy(step, side, c, True).wait_recv(), split)

    def relays(act):
        for side in (0, 1):
            pl.when(me["lon"] == (0 if side == 0 else n_lon - 1))(functools.partial(act, side))

    def forward(step, c):
        def act(side):
            to_relay(step, side, c).wait_recv()
            from_relay(step, side, c).start()

        relays(act)

    def lev_copy(step, side, arriving=False):
        slot = step % 2
        landing = side if arriving else 1 - side
        return pltpu.make_async_remote_copy(
            src_ref=lev_out.at[slot, side],
            dst_ref=lev_in.at[slot, landing],
            send_sem=lev_send.at[slot, side],
            recv_sem=lev_recv.at[slot, landing],
            device_id=beside("lev", side),
            device_id_type=MESH,
        )

    def send_chunk(step, c):
        start_lon(step, c)
        both("lat", lambda side: lat_copy(step, side, c).start())

    def sent_chunk(step, c):
        sent_lon(step, c)
        both("lat", lambda side: lat_copy(step, side, c).wait_send())

    def send_lev(step, side):
        state = states[step % 2]
        row = PAD if side == 0 else PAD + K - 1

        @pl.loop(1, J + 1)
        def _(p):
            lev_out[step % 2, side, p - 1] = state[p, 1 : I + 1, row : row + 1, :]

        lev_copy(step, side).start()

    def take_lev(step, side):
        state = states[step % 2]
        row = PAD - 1 if side == 0 else PAD + K
        lev_copy(step, side, True).wait_recv()

        @pl.loop(1, J + 1)
        def _(p):
            state[p, 1 : I + 1, row : row + 1, :] = lev_in[step % 2, side, p - 1]

    pl.loop(0, EARLY)(lambda c: send_chunk(0, c))
    pl.loop(0, chunks)(lambda c: forward(0, c))
    pl.loop(EARLY, chunks)(lambda c: send_chunk(0, c))

    def clear(axis, side):
        for state in states:
            if axis == "lat":
                target = 0 if side == 0 else J + 1

                @pl.loop(1, I + 1)
                def _(i):
                    state[target, i, PAD : PAD + K, :] = jnp.zeros((K, M), jnp.float32)
            elif axis == "lon":
                target = 0 if side == 0 else I + 1
                for p in range(1, J + 1):
                    state[p, target, PAD : PAD + K, :] = jnp.zeros((K, M), jnp.float32)
            else:
                target = PAD - 1 if side == 0 else PAD + K

                @pl.loop(1, J + 1)
                def _(p):
                    state[p, 1 : I + 1, target : target + 1, :] = jnp.zeros(
                        (I, 1, M), jnp.float32
                    )

    for axis in ("lat", "lon", "lev"):
        for side in (0, 1):
            pl.when(jnp.logical_not(has(axis, side)))(functools.partial(clear, axis, side))

    for j in range(J):
        load(0, j).wait()
    both("lev", lambda side: send_lev(0, side))
    for j in range(J):
        load(1, j).wait()
        load(2, j).wait()

    def update(step, c, first, count):
        now, later = states[step % 2], states[(step + 1) % 2]
        last = step == STEPS - 1
        start = pl.multiple_of(PAD + c * CHUNK, CHUNK)
        here = pl.ds(start, CHUNK)
        inner = inside(c)

        def row(i, carry):
            past, mid, sums = carry
            coming = tuple(now[first + n, i + 1, here, :] for n in range(count))
            column = (now[first - 1, i, here, :],) + mid + (now[first + count, i, here, :],)
            out = []
            for n in range(count):
                p = first + n
                spread = (
                    (column[n] + column[n + 2])
                    + (past[n] + coming[n])
                    + (
                        now[p, i, pl.ds(start - 1, CHUNK), :]
                        + now[p, i, pl.ds(start + 1, CHUNK), :]
                    )
                    - 6.0 * mid[n]
                )
                new = (
                    mid[n]
                    + coef[p - 1, i - 1, inner, :] * spread
                    + source[p - 1, i - 1, inner, :]
                )
                if last:
                    end[p - 1, i - 1, inner, :] = new
                else:
                    later[p, i, here, :] = new
                out.append(new)
            if last:
                sums = tuple(total + new for total, new in zip(sums, out))
            return mid, coming, sums

        zero = jnp.zeros((CHUNK, M), jnp.float32)
        _, _, sums = lax.fori_loop(
            1,
            I + 1,
            row,
            (
                tuple(now[first + n, 0, here, :] for n in range(count)),
                tuple(now[first + n, 1, here, :] for n in range(count)),
                (zero,) * count if last else (),
            ),
            unroll=2 if count > 1 else 4,
        )
        return sums

    my_half = pl.ds(half * my_core, half)
    other_half = pl.ds(half * (1 - my_core), half)
    inner_plane = 1 + me["lat"]
    edge_plane = jnp.where(me["lat"] == 0, J, 1)
    partner = {"lon": me["lon"] + 1 - 2 * my_core}

    def mate_copy(c):
        return pltpu.make_async_remote_copy(
            src_ref=total.at[:, inside(c)],
            dst_ref=mate.at[:, inside(c)],
            send_sem=mate_send.at[c],
            recv_sem=mate_recv.at[c],
            device_id=partner,
            device_id_type=MESH,
        )

    def chip_copy(target, c, arriving=None):
        sender = my_chip if arriving is None else arriving
        return pltpu.make_async_remote_copy(
            src_ref=chip.at[:, inside(c)],
            dst_ref=chip_in.at[sender, :, inside(c)],
            send_sem=chip_send.at[target, c],
            recv_sem=chip_recv.at[sender, c],
            device_id={"lon": target * CORES + my_core},
            device_id_type=MESH,
        )

    def half_copy():
        return pltpu.make_async_remote_copy(
            src_ref=mine,
            dst_ref=theirs,
            send_sem=half_sem.at[0],
            recv_sem=half_sem.at[1],
            device_id=partner,
            device_id_type=MESH,
        )

    def edge_copy(target, arriving=None):
        sender = me["lon"] if arriving is None else arriving
        return pltpu.make_async_remote_copy(
            src_ref=edge,
            dst_ref=edge_in.at[sender],
            send_sem=edge_send.at[target],
            recv_sem=edge_recv.at[sender],
            device_id={"lon": jnp.int32(target)},
            device_id_type=MESH,
        )

    def later_chips(act):
        for other in range(1, n_chips):
            pl.when(other > my_chip)(functools.partial(act, other))

    def earlier_chips(act):
        for other in range(n_chips - 1):
            pl.when(other < my_chip)(functools.partial(act, other))

    def later_cores(act):
        for other in range(1, n_lon):
            pl.when(other > me["lon"])(functools.partial(act, other))

    def earlier_cores(act):
        for other in range(n_lon - 1):
            pl.when(other < me["lon"])(functools.partial(act, other))

    def share(c):
        mate_copy(c).wait()
        chip[:, inside(c), :] = total[my_half, inside(c), :] + mate[my_half, inside(c), :]
        later_chips(lambda other: chip_copy(other, c).start())

    def take_lon(step, c):
        arrived_lon(step, c)
        for side, end_chunk in ((0, 0), (1, chunks - 1)):
            pl.when(jnp.logical_and(c == end_chunk, has("lev", side)))(
                functools.partial(take_lev, step, side)
            )

    def send_lat(step, c):
        both("lat", lambda side: lat_copy(step, side, c).start())

    def take_lat(step, c):
        both("lat", lambda side: lat_copy(step, side, c, True).wait_recv())

    for step in range(STEPS - 1):
        if 0 < step < RELAYS:
            forward(step, chunks - 1)

        @pl.loop(0, chunks)
        def _(c):
            if step > 0:
                sent_chunk(step - 1, c)
            take_lon(step, c)
            take_lat(step, c)
            update(step, c, 1, J)
            if step + 1 < RELAYS:
                pl.when(c > 0)(lambda: forward(step + 1, c - 1))
            if step < STEPS - 2:
                send_chunk(step + 1, c)
            else:
                start_lon(step + 1, c)
                pl.when(c < EARLY)(lambda: send_lat(step + 1, c))
            for side, end_chunk in ((0, 0), (1, chunks - 1)):

                def pass_on(side=side):
                    if step > 0:
                        lev_copy(step - 1, side).wait_send()
                    send_lev(step + 1, side)

                pl.when(jnp.logical_and(c == end_chunk, has("lev", side)))(pass_on)

    last = STEPS - 1
    for c in range(EARLY, chunks):
        send_lat(last, c)

    @pl.loop(0, chunks)
    def _(c):
        sent_chunk(last - 1, c)
        take_lon(last, c)
        sums = update(last, c, inner_plane, J - 1)
        for n in range(J - 1):
            total[inner_plane - 1 + n, inside(c), :] = sums[n]

    def edge_step(c):
        take_lat(last, c)
        return update(last, c, edge_plane, 1)[0]

    tail = chunks - 1
    total[edge_plane - 1, inside(tail), :] = jnp.zeros((CHUNK, M), jnp.float32)
    mate_copy(tail).start()

    @pl.loop(0, tail)
    def _(c):
        total[edge_plane - 1, inside(c), :] = edge_step(c)
        mate_copy(c).start()
        pl.when(c > 0)(lambda: share(c - 1))

    share(tail)
    share(tail - 1)
    edge[...] = edge_step(tail)
    later_cores(lambda other: edge_copy(other).start())

    mine[...] = jnp.zeros(mine.shape, jnp.float32)

    def add_chip(other):
        for c in range(chunks):
            chip_copy(0, c, other).wait_recv()
        mine[...] += chip_in[other]

    earlier_chips(add_chip)
    half_copy().start()
    before[my_half] = mine[...]
    half_copy().wait()
    before[other_half] = theirs[...]

    @pl.when(my_core == 1)
    def _():
        before[...] += mate[...]

    def add_edge(other):
        edge_copy(0, other).wait_recv()
        before[edge_plane - 1, inside(tail), :] += edge_in[other]

    earlier_cores(add_edge)

    for step in (STEPS - 2, STEPS - 1):
        both("lev", lambda side: lev_copy(step, side).wait_send())
    for c in range(chunks):
        sent_chunk(STEPS - 1, c)
        later_chips(lambda other: chip_copy(other, c).wait_send())
    later_cores(lambda other: edge_copy(other).wait_send())
    for step in range(RELAYS):
        pl.loop(0, chunks)(
            lambda c: relays(lambda side: from_relay(step, side, c).wait_send())
        )


def totals_kernel(scale, x, before, totals, end, sums, end_sem, sums_sem):
    J, I = x.shape[:2]

    def out(which, j):
        src, dst, sem = ((x, end, end_sem), (sums, totals, sums_sem))[which]
        return pltpu.make_async_copy(src.at[j], dst.at[j], sem.at[j])

    for j in range(J):
        out(0, j).start()

    @pl.loop(0, J)
    def _(j):
        def row(i, total):
            total = total + x[j, i]
            sums[j, i] = total * scale
            return total

        lax.fori_loop(0, I, row, before[j], unroll=4)
        out(1, j).start()

    for j in range(J):
        out(0, j).wait()
        out(1, j).wait()


def per_device(sizes, initial_state, scaled_diffusivity, scaled_forcing):
    J, I, K, M = initial_state.shape
    chunks = K // CHUNK
    n_lon = sizes["lon"]
    n_chips = n_lon // CORES
    half = J // CORES
    f32 = jnp.float32
    vmem = lambda *shape: pltpu.VMEM(shape, f32)
    sem = lambda *shape: pltpu.SemaphoreType.DMA(shape)
    hbm = pl.BlockSpec(memory_space=pltpu.HBM)
    local = pl.BlockSpec(memory_space=pltpu.VMEM)
    end, before = pl.pallas_call(
        functools.partial(steps_kernel, sizes),
        out_shape=(vmem(J, I, K, M), vmem(J, K, M)),
        in_specs=[hbm] * 3,
        out_specs=(local, local),
        scratch_shapes=[
            vmem(J + 2, I + 2, K + 2 * PAD, M),
            vmem(J + 2, I + 2, K + 2 * PAD, M),
            vmem(J, I, K, M),
            vmem(J, I, K, M),
            vmem(2, 2, J, I, 1, M),
            vmem(2, 2, J, I, 1, M),
            vmem(J, K, M),
            vmem(J, K, M),
            vmem(half, K, M),
            vmem(n_chips, half, K, M),
            vmem(half, K, M),
            vmem(half, K, M),
            vmem(CHUNK, M),
            vmem(n_lon, CHUNK, M),
            vmem(RELAYS, half, K, M),
            sem(2, 2, chunks),
            sem(2, 2, chunks),
            sem(2, 2, chunks),
            sem(2, 2, chunks),
            sem(2, 2),
            sem(2, 2),
            sem(3, J),
            sem(chunks),
            sem(chunks),
            sem(n_chips, chunks),
            sem(n_chips, chunks),
            sem(2),
            sem(n_lon),
            sem(n_lon),
            sem(RELAYS, chunks),
            sem(RELAYS, chunks),
            sem(RELAYS, chunks),
            sem(RELAYS, chunks),
        ],
        compiler_params=pltpu.CompilerParams(
            collective_id=0, has_side_effects=True, vmem_limit_bytes=50 * 2**20
        ),
        name="steps",
    )(initial_state, scaled_diffusivity, scaled_forcing)

    return pl.pallas_call(
        functools.partial(totals_kernel, 1.0 / (I * n_lon)),
        out_shape=(jax.ShapeDtypeStruct((J, I, K, M), f32),) * 2,
        in_specs=[local, local],
        out_specs=(hbm, hbm),
        scratch_shapes=[vmem(J, I, K, M), sem(J), sem(J)],
        compiler_params=pltpu.CompilerParams(vmem_limit_bytes=20 * 2**20),
        name="totals",
    )(end, before)


def solution(mesh):
    spec = P("lat", "lon", "lev", None)
    return jax.shard_map(
        functools.partial(per_device, dict(mesh.shape)),
        mesh=mesh,
        in_specs=(spec,) * 3,
        out_specs=(spec,) * 2,
        check_vma=False,
    )
```

```python
import functools

import jax
import jax.numpy as jnp
from jax import lax
from jax.experimental import pallas as pl
from jax.experimental.pallas import tpu as pltpu
from jax.sharding import PartitionSpec as P

STEPS = 4
PAD = 8
CHUNK = 8
CORES = 2
EARLY = 2
AHEAD = 4
MESH = pl.DeviceIdType.MESH


def steps_kernel(
    sizes, x, d, f, end, before, even, odd, coef, source,
    lev_out, lev_in, total, mate, chip, chip_in, mine, theirs, edge, edge_in, relay,
    lat_send, lat_recv, lon_send, lon_recv, lev_send, lev_recv,
    load_sem, mate_send, mate_recv, chip_send, chip_recv, half_sem, edge_send, edge_recv,
    relay_send, relay_recv, pass_send, pass_recv,
):
    J, I, K, M = x.shape
    chunks = K // CHUNK
    states = (even, odd)
    me = {axis: lax.axis_index(axis) for axis in sizes}
    n_lon = sizes["lon"]
    n_chips = n_lon // CORES
    my_chip = me["lon"] // CORES
    my_core = me["lon"] % CORES
    half = J // CORES
    rows = pl.ds(1, I)
    levels = pl.ds(PAD, K)
    planes = pl.ds(1, J)

    def has(axis, side):
        return me[axis] > 0 if side == 0 else me[axis] < sizes[axis] - 1

    def beside(axis, side):
        return {axis: me[axis] - 1 if side == 0 else me[axis] + 1}

    def both(axis, act):
        if sizes[axis] > 1:
            for side in (0, 1):
                pl.when(has(axis, side))(functools.partial(act, side))

    def load(which, j):
        src, dst = (
            (x.at[j], even.at[j + 1, rows, levels]),
            (d.at[j], coef.at[j]),
            (f.at[j], source.at[j]),
        )[which]
        return pltpu.make_async_copy(src, dst, load_sem.at[which, j])

    barrier = pltpu.get_barrier_semaphore()
    count = jnp.int32(n_lon - 1)

    def greet(target):
        pl.semaphore_signal(barrier, inc=1, device_id=target, device_id_type=MESH)

    for axis in ("lat", "lev"):
        both(axis, lambda side, axis=axis: greet(beside(axis, side)))
        if sizes[axis] > 1:
            count = count + has(axis, 0).astype(jnp.int32) + has(axis, 1).astype(jnp.int32)
    for other in range(n_lon):
        pl.when(other != me["lon"])(lambda other=other: greet({"lon": jnp.int32(other)}))
    for which in range(3):
        for j in range(J):
            load(which, j).start()

    pl.semaphore_wait(barrier, count)

    def inside(c):
        return pl.ds(pl.multiple_of(c * CHUNK, CHUNK), CHUNK)

    def padded(c):
        return pl.ds(pl.multiple_of(PAD + c * CHUNK, CHUNK), CHUNK)

    def lat_copy(step, side, c, arriving=False):
        slot = step % 2
        state = states[slot]
        plane, target = (1, J + 1) if side == 0 else (J, 0)
        if arriving:
            target = 0 if side == 0 else J + 1
        if step == 0:
            src = x.at[plane - 1, :, inside(c)]
        else:
            src = state.at[plane, rows, padded(c)]
        return pltpu.make_async_remote_copy(
            src_ref=src,
            dst_ref=state.at[target, rows, padded(c)],
            send_sem=lat_send.at[slot, side, c],
            recv_sem=lat_recv.at[slot, side if arriving else 1 - side, c],
            device_id=beside("lat", side),
            device_id_type=MESH,
        )

    def lon_copy(step, side, c, arriving=False, count=J):
        slot = step % 2
        state = states[slot]
        row, target = (1, I + 1) if side == 0 else (I, 0)
        if arriving:
            target = 0 if side == 0 else I + 1
        if step == 0:
            src = x.at[pl.ds(0, count), row - 1, inside(c)]
        else:
            src = state.at[pl.ds(1, count), row, padded(c)]
        return pltpu.make_async_remote_copy(
            src_ref=src,
            dst_ref=state.at[pl.ds(1, count), target, padded(c)],
            send_sem=lon_send.at[slot, side, c],
            recv_sem=lon_recv.at[slot, side if arriving else 1 - side, c],
            device_id=beside("lon", side),
            device_id_type=MESH,
        )

    def to_relay(step, side, c):
        row = 1 if side == 0 else I
        if step == 0:
            src = x.at[pl.ds(half, half), row - 1, inside(c)]
        else:
            src = states[step % 2].at[pl.ds(1 + half, half), row, padded(c)]
        return pltpu.make_async_remote_copy(
            src_ref=src,
            dst_ref=relay.at[step, :, inside(c)],
            send_sem=relay_send.at[step, c],
            recv_sem=relay_recv.at[step, c],
            device_id={"lon": jnp.int32(0 if side == 0 else n_lon - 1)},
            device_id_type=MESH,
        )

    def from_relay(step, side, c):
        target = I + 1 if side == 0 else 0
        return pltpu.make_async_remote_copy(
            src_ref=relay.at[step, :, inside(c)],
            dst_ref=states[step % 2].at[pl.ds(1 + half, half), target, padded(c)],
            send_sem=pass_send.at[step, c],
            recv_sem=pass_recv.at[step, c],
            device_id={"lon": jnp.int32(n_lon // 2 - 1 if side == 0 else n_lon // 2)},
            device_id_type=MESH,
        )

    def relay_sides(step):
        return (0, 1) if step < STEPS - 1 else (1,)

    def lon_each(step, whole, split, arriving=False):
        for side in (0, 1):
            halved = me["lon"] == (n_lon // 2 if side == 0 else n_lon // 2 - 1)
            if (1 - side if arriving else side) in relay_sides(step):
                pl.when(jnp.logical_and(has("lon", side), jnp.logical_not(halved)))(
                    functools.partial(whole, side)
                )
                pl.when(halved)(functools.partial(split, side))
            else:
                pl.when(has("lon", side))(functools.partial(whole, side))

    def start_lon(step, c):
        def split(side):
            to_relay(step, side, c).start()
            lon_copy(step, side, c, count=half).start()

        lon_each(step, lambda side: lon_copy(step, side, c).start(), split)

    def sent_lon(step, c):
        def split(side):
            to_relay(step, side, c).wait_send()
            lon_copy(step, side, c, count=half).wait_send()

        lon_each(step, lambda side: lon_copy(step, side, c).wait_send(), split)

    def arrived_lon(step, c):
        def split(side):
            from_relay(step, 1 - side, c).wait_recv()
            lon_copy(step, side, c, True, half).wait_recv()

        lon_each(step, lambda side: lon_copy(step, side, c, True).wait_recv(), split, True)

    def relays(step, act):
        for side in relay_sides(step):
            pl.when(me["lon"] == (0 if side == 0 else n_lon - 1))(functools.partial(act, side))

    def forward(step, c):
        def act(side):
            to_relay(step, side, c).wait_recv()
            from_relay(step, side, c).start()

        relays(step, act)

    def lev_copy(step, side, arriving=False):
        slot = step % 2
        landing = side if arriving else 1 - side
        return pltpu.make_async_remote_copy(
            src_ref=lev_out.at[slot, side],
            dst_ref=lev_in.at[slot, landing],
            send_sem=lev_send.at[slot, side],
            recv_sem=lev_recv.at[slot, landing],
            device_id=beside("lev", side),
            device_id_type=MESH,
        )

    def send_chunk(step, c):
        start_lon(step, c)
        both("lat", lambda side: lat_copy(step, side, c).start())

    def sent_chunk(step, c):
        sent_lon(step, c)
        both("lat", lambda side: lat_copy(step, side, c).wait_send())

    def send_lev(step, side):
        state = states[step % 2]
        row = PAD if side == 0 else PAD + K - 1

        @pl.loop(1, J + 1)
        def _(p):
            lev_out[step % 2, side, p - 1] = state[p, 1 : I + 1, row : row + 1, :]

        lev_copy(step, side).start()

    def take_lev(step, side):
        state = states[step % 2]
        row = PAD - 1 if side == 0 else PAD + K
        lev_copy(step, side, True).wait_recv()

        @pl.loop(1, J + 1)
        def _(p):
            state[p, 1 : I + 1, row : row + 1, :] = lev_in[step % 2, side, p - 1]

    pl.loop(0, EARLY)(lambda c: send_chunk(0, c))
    pl.loop(0, chunks)(lambda c: forward(0, c))
    pl.loop(EARLY, chunks)(lambda c: send_chunk(0, c))

    def clear(axis, side):
        for state in states:
            if axis == "lat":
                target = 0 if side == 0 else J + 1

                @pl.loop(1, I + 1)
                def _(i):
                    state[target, i, PAD : PAD + K, :] = jnp.zeros((K, M), jnp.float32)
            elif axis == "lon":
                target = 0 if side == 0 else I + 1
                for p in range(1, J + 1):
                    state[p, target, PAD : PAD + K, :] = jnp.zeros((K, M), jnp.float32)
            else:
                target = PAD - 1 if side == 0 else PAD + K

                @pl.loop(1, J + 1)
                def _(p):
                    state[p, 1 : I + 1, target : target + 1, :] = jnp.zeros(
                        (I, 1, M), jnp.float32
                    )

    for axis in ("lat", "lon", "lev"):
        for side in (0, 1):
            pl.when(jnp.logical_not(has(axis, side)))(functools.partial(clear, axis, side))

    for j in range(J):
        load(0, j).wait()
    both("lev", lambda side: send_lev(0, side))
    for j in range(J):
        load(1, j).wait()
        load(2, j).wait()

    def update(step, c, first, count):
        now, later = states[step % 2], states[(step + 1) % 2]
        last = step == STEPS - 1
        start = pl.multiple_of(PAD + c * CHUNK, CHUNK)
        here = pl.ds(start, CHUNK)
        inner = inside(c)

        def row(i, carry):
            past, mid, sums = carry
            coming = tuple(now[first + n, i + 1, here, :] for n in range(count))
            column = (now[first - 1, i, here, :],) + mid + (now[first + count, i, here, :],)
            out = []
            for n in range(count):
                p = first + n
                spread = (
                    (column[n] + column[n + 2])
                    + (past[n] + coming[n])
                    + (
                        now[p, i, pl.ds(start - 1, CHUNK), :]
                        + now[p, i, pl.ds(start + 1, CHUNK), :]
                    )
                    - 6.0 * mid[n]
                )
                new = (
                    mid[n]
                    + coef[p - 1, i - 1, inner, :] * spread
                    + source[p - 1, i - 1, inner, :]
                )
                if last:
                    end[p - 1, i - 1, inner, :] = new
                else:
                    later[p, i, here, :] = new
                out.append(new)
            if last:
                sums = tuple(total + new for total, new in zip(sums, out))
            return mid, coming, sums

        zero = jnp.zeros((CHUNK, M), jnp.float32)
        _, _, sums = lax.fori_loop(
            1,
            I + 1,
            row,
            (
                tuple(now[first + n, 0, here, :] for n in range(count)),
                tuple(now[first + n, 1, here, :] for n in range(count)),
                (zero,) * count if last else (),
            ),
            unroll=2 if count > 1 else 4,
        )
        return sums

    my_half = pl.ds(half * my_core, half)
    other_half = pl.ds(half * (1 - my_core), half)
    inner_plane = 1 + me["lat"]
    edge_plane = jnp.where(me["lat"] == 0, J, 1)
    partner = {"lon": me["lon"] + 1 - 2 * my_core}

    def mate_copy(c):
        return pltpu.make_async_remote_copy(
            src_ref=total.at[:, inside(c)],
            dst_ref=mate.at[:, inside(c)],
            send_sem=mate_send.at[c],
            recv_sem=mate_recv.at[c],
            device_id=partner,
            device_id_type=MESH,
        )

    def chip_copy(target, c, arriving=None):
        sender = my_chip if arriving is None else arriving
        return pltpu.make_async_remote_copy(
            src_ref=chip.at[:, inside(c)],
            dst_ref=chip_in.at[sender, :, inside(c)],
            send_sem=chip_send.at[target, c],
            recv_sem=chip_recv.at[sender, c],
            device_id={"lon": target * CORES + my_core},
            device_id_type=MESH,
        )

    def half_copy():
        return pltpu.make_async_remote_copy(
            src_ref=mine,
            dst_ref=theirs,
            send_sem=half_sem.at[0],
            recv_sem=half_sem.at[1],
            device_id=partner,
            device_id_type=MESH,
        )

    def edge_copy(target, arriving=None):
        sender = me["lon"] if arriving is None else arriving
        return pltpu.make_async_remote_copy(
            src_ref=edge,
            dst_ref=edge_in.at[sender],
            send_sem=edge_send.at[target],
            recv_sem=edge_recv.at[sender],
            device_id={"lon": jnp.int32(target)},
            device_id_type=MESH,
        )

    def later_chips(act):
        for other in range(1, n_chips):
            pl.when(other > my_chip)(functools.partial(act, other))

    def earlier_chips(act):
        for other in range(n_chips - 1):
            pl.when(other < my_chip)(functools.partial(act, other))

    def later_cores(act):
        for other in range(1, n_lon):
            pl.when(other > me["lon"])(functools.partial(act, other))

    def earlier_cores(act):
        for other in range(n_lon - 1):
            pl.when(other < me["lon"])(functools.partial(act, other))

    def share(c):
        mate_copy(c).wait()
        chip[:, inside(c), :] = total[my_half, inside(c), :] + mate[my_half, inside(c), :]
        later_chips(lambda other: chip_copy(other, c).start())

    def take_lon(step, c):
        arrived_lon(step, c)
        for side, end_chunk in ((0, 0), (1, chunks - 1)):
            pl.when(jnp.logical_and(c == end_chunk, has("lev", side)))(
                functools.partial(take_lev, step, side)
            )

    def send_lat(step, c):
        both("lat", lambda side: lat_copy(step, side, c).start())

    def take_lat(step, c):
        both("lat", lambda side: lat_copy(step, side, c, True).wait_recv())

    for step in range(STEPS - 1):
        if step > 0:
            forward(step, chunks - 1)

        @pl.loop(0, chunks)
        def _(c):
            if step > 0:
                sent_chunk(step - 1, c)
            take_lon(step, c)
            take_lat(step, c)
            update(step, c, 1, J)
            if step + 1 < STEPS - 1:
                pl.when(c > 0)(lambda: forward(step + 1, c - 1))
            if step < STEPS - 2:
                send_chunk(step + 1, c)
            else:
                start_lon(step + 1, c)
                pl.when(c < EARLY)(lambda: send_lat(step + 1, c))
            for side, end_chunk in ((0, 0), (1, chunks - 1)):

                def pass_on(side=side):
                    if step > 0:
                        lev_copy(step - 1, side).wait_send()
                    send_lev(step + 1, side)

                pl.when(jnp.logical_and(c == end_chunk, has("lev", side)))(pass_on)

    last = STEPS - 1
    for c in range(EARLY, AHEAD):
        send_lat(last, c)
    pl.loop(0, chunks)(lambda c: forward(last, c))
    for c in range(AHEAD, chunks):
        send_lat(last, c)

    @pl.loop(0, chunks)
    def _(c):
        sent_chunk(last - 1, c)
        take_lon(last, c)
        sums = update(last, c, inner_plane, J - 1)
        for n in range(J - 1):
            total[inner_plane - 1 + n, inside(c), :] = sums[n]

    def edge_step(c):
        take_lat(last, c)
        return update(last, c, edge_plane, 1)[0]

    tail = chunks - 1
    total[edge_plane - 1, inside(tail), :] = jnp.zeros((CHUNK, M), jnp.float32)
    mate_copy(tail).start()

    @pl.loop(0, tail)
    def _(c):
        total[edge_plane - 1, inside(c), :] = edge_step(c)
        mate_copy(c).start()
        pl.when(c > 0)(lambda: share(c - 1))

    share(tail)
    share(tail - 1)
    edge[...] = edge_step(tail)
    later_cores(lambda other: edge_copy(other).start())

    mine[...] = jnp.zeros(mine.shape, jnp.float32)

    def add_chip(other):
        for c in range(chunks):
            chip_copy(0, c, other).wait_recv()
        mine[...] += chip_in[other]

    earlier_chips(add_chip)
    half_copy().start()
    before[my_half] = mine[...]
    half_copy().wait()
    before[other_half] = theirs[...]

    @pl.when(my_core == 1)
    def _():
        before[...] += mate[...]

    def add_edge(other):
        edge_copy(0, other).wait_recv()
        before[edge_plane - 1, inside(tail), :] += edge_in[other]

    earlier_cores(add_edge)

    for step in (STEPS - 2, STEPS - 1):
        both("lev", lambda side: lev_copy(step, side).wait_send())
    for c in range(chunks):
        sent_chunk(STEPS - 1, c)
        later_chips(lambda other: chip_copy(other, c).wait_send())
    later_cores(lambda other: edge_copy(other).wait_send())
    for step in range(STEPS):
        pl.loop(0, chunks)(
            lambda c: relays(step, lambda side: from_relay(step, side, c).wait_send())
        )


def totals_kernel(scale, x, before, totals, end, sums, end_sem, sums_sem):
    J, I = x.shape[:2]

    def out(which, j):
        src, dst, sem = ((x, end, end_sem), (sums, totals, sums_sem))[which]
        return pltpu.make_async_copy(src.at[j], dst.at[j], sem.at[j])

    for j in range(J):
        out(0, j).start()

    @pl.loop(0, J)
    def _(j):
        def row(i, total):
            total = total + x[j, i]
            sums[j, i] = total * scale
            return total

        lax.fori_loop(0, I, row, before[j], unroll=4)
        out(1, j).start()

    for j in range(J):
        out(0, j).wait()
        out(1, j).wait()


def per_device(sizes, initial_state, scaled_diffusivity, scaled_forcing):
    J, I, K, M = initial_state.shape
    chunks = K // CHUNK
    n_lon = sizes["lon"]
    n_chips = n_lon // CORES
    half = J // CORES
    f32 = jnp.float32
    vmem = lambda *shape: pltpu.VMEM(shape, f32)
    sem = lambda *shape: pltpu.SemaphoreType.DMA(shape)
    hbm = pl.BlockSpec(memory_space=pltpu.HBM)
    local = pl.BlockSpec(memory_space=pltpu.VMEM)
    end, before = pl.pallas_call(
        functools.partial(steps_kernel, sizes),
        out_shape=(vmem(J, I, K, M), vmem(J, K, M)),
        in_specs=[hbm] * 3,
        out_specs=(local, local),
        scratch_shapes=[
            vmem(J + 2, I + 2, K + 2 * PAD, M),
            vmem(J + 2, I + 2, K + 2 * PAD, M),
            vmem(J, I, K, M),
            vmem(J, I, K, M),
            vmem(2, 2, J, I, 1, M),
            vmem(2, 2, J, I, 1, M),
            vmem(J, K, M),
            vmem(J, K, M),
            vmem(half, K, M),
            vmem(n_chips, half, K, M),
            vmem(half, K, M),
            vmem(half, K, M),
            vmem(CHUNK, M),
            vmem(n_lon, CHUNK, M),
            vmem(STEPS, half, K, M),
            sem(2, 2, chunks),
            sem(2, 2, chunks),
            sem(2, 2, chunks),
            sem(2, 2, chunks),
            sem(2, 2),
            sem(2, 2),
            sem(3, J),
            sem(chunks),
            sem(chunks),
            sem(n_chips, chunks),
            sem(n_chips, chunks),
            sem(2),
            sem(n_lon),
            sem(n_lon),
            sem(STEPS, chunks),
            sem(STEPS, chunks),
            sem(STEPS, chunks),
            sem(STEPS, chunks),
        ],
        compiler_params=pltpu.CompilerParams(
            collective_id=0, has_side_effects=True, vmem_limit_bytes=50 * 2**20
        ),
        name="steps",
    )(initial_state, scaled_diffusivity, scaled_forcing)

    return pl.pallas_call(
        functools.partial(totals_kernel, 1.0 / (I * n_lon)),
        out_shape=(jax.ShapeDtypeStruct((J, I, K, M), f32),) * 2,
        in_specs=[local, local],
        out_specs=(hbm, hbm),
        scratch_shapes=[vmem(J, I, K, M), sem(J), sem(J)],
        compiler_params=pltpu.CompilerParams(vmem_limit_bytes=20 * 2**20),
        name="totals",
    )(end, before)


def solution(mesh):
    spec = P("lat", "lon", "lev", None)
    return jax.shard_map(
        functools.partial(per_device, dict(mesh.shape)),
        mesh=mesh,
        in_specs=(spec,) * 3,
        out_specs=(spec,) * 2,
        check_vma=False,
    )
```

```python
import functools

import jax
import jax.numpy as jnp
from jax import lax
from jax.experimental import pallas as pl
from jax.experimental.pallas import tpu as pltpu
from jax.sharding import PartitionSpec as P

STEPS = 4
PAD = 8
CHUNK = 8
CORES = 2
EARLY = 2
AHEAD = 4
FIRST = 4
ROUNDS = 4
MESH = pl.DeviceIdType.MESH


def steps_kernel(
    sizes, x, d, f, end, before, even, odd, coef, source,
    lev_out, lev_in, total, mate, chip, chip_in, mine, theirs, edge, edge_in, relay,
    lat_send, lat_recv, lon_send, lon_recv, lev_send, lev_recv,
    load_sem, mate_send, mate_recv, chip_send, chip_recv, half_sem, edge_send, edge_recv,
    relay_send, relay_recv, pass_send, pass_recv, rounds,
):
    J, I, K, M = x.shape
    chunks = K // CHUNK
    states = (even, odd)
    me = {axis: lax.axis_index(axis) for axis in sizes}
    n_lon = sizes["lon"]
    n_chips = n_lon // CORES
    my_chip = me["lon"] // CORES
    my_core = me["lon"] % CORES
    half = J // CORES
    rows = pl.ds(1, I)
    levels = pl.ds(PAD, K)
    planes = pl.ds(1, J)

    def has(axis, side):
        return me[axis] > 0 if side == 0 else me[axis] < sizes[axis] - 1

    def beside(axis, side):
        return {axis: me[axis] - 1 if side == 0 else me[axis] + 1}

    def both(axis, act):
        if sizes[axis] > 1:
            for side in (0, 1):
                pl.when(has(axis, side))(functools.partial(act, side))

    def load(which, j):
        src, dst = (
            (x.at[j], even.at[j + 1, rows, levels]),
            (d.at[j], coef.at[j]),
            (f.at[j], source.at[j]),
        )[which]
        return pltpu.make_async_copy(src, dst, load_sem.at[which, j])

    barrier = pltpu.get_barrier_semaphore()
    lev_half, lon_half = sizes["lev"] // 2, n_lon // 2
    across, deep = me["lon"] // CORES % 2, me["lon"] // lon_half
    ring, lap = me["lev"] % lev_half, me["lev"] // lev_half
    side_x = 2 * across + me["lat"]
    side_z = 2 * lap + deep
    spot = lambda axis, index: {axis: index}
    near = (
        (jnp.bool_(True), spot("lat", 1 - me["lat"])),
        (jnp.bool_(True), spot("lon", me["lon"] + 1 - 2 * my_core)),
        (jnp.bool_(True), spot("lon", me["lon"] + lon_half - 2 * lon_half * deep)),
        (ring > 0, spot("lev", me["lev"] - 1)),
        (ring < lev_half - 1, spot("lev", me["lev"] + 1)),
        (
            jnp.logical_or(side_x == 1, side_x == 2),
            {"lat": 1 - me["lat"], "lon": me["lon"] + CORES - 2 * CORES * across},
        ),
        (
            jnp.logical_or(side_z == 1, side_z == 2),
            {
                "lon": me["lon"] + lon_half - 2 * lon_half * deep,
                "lev": me["lev"] + lev_half - 2 * lev_half * lap,
            },
        ),
    )
    peers = sum(there.astype(jnp.int32) for there, _ in near)

    def meet(semaphore):
        for there, target in near:
            pl.when(there)(
                lambda target=target: pl.semaphore_signal(
                    semaphore, inc=1, device_id=target, device_id_type=MESH
                )
            )
        pl.semaphore_wait(semaphore, peers)

    meet(barrier)

    def inside(c):
        return pl.ds(pl.multiple_of(c * CHUNK, CHUNK), CHUNK)

    def padded(c):
        return pl.ds(pl.multiple_of(PAD + c * CHUNK, CHUNK), CHUNK)

    def lat_copy(step, side, c, arriving=False):
        slot = step % 2
        state = states[slot]
        plane, target = (1, J + 1) if side == 0 else (J, 0)
        if arriving:
            target = 0 if side == 0 else J + 1
        if step == 0:
            src = x.at[plane - 1, :, inside(c)]
        else:
            src = state.at[plane, rows, padded(c)]
        return pltpu.make_async_remote_copy(
            src_ref=src,
            dst_ref=state.at[target, rows, padded(c)],
            send_sem=lat_send.at[slot, side, c],
            recv_sem=lat_recv.at[slot, side if arriving else 1 - side, c],
            device_id=beside("lat", side),
            device_id_type=MESH,
        )

    def lon_copy(step, side, c, arriving=False, count=J):
        slot = step % 2
        state = states[slot]
        row, target = (1, I + 1) if side == 0 else (I, 0)
        if arriving:
            target = 0 if side == 0 else I + 1
        if step == 0:
            src = x.at[pl.ds(0, count), row - 1, inside(c)]
        else:
            src = state.at[pl.ds(1, count), row, padded(c)]
        return pltpu.make_async_remote_copy(
            src_ref=src,
            dst_ref=state.at[pl.ds(1, count), target, padded(c)],
            send_sem=lon_send.at[slot, side, c],
            recv_sem=lon_recv.at[slot, side if arriving else 1 - side, c],
            device_id=beside("lon", side),
            device_id_type=MESH,
        )

    def to_relay(step, side, c):
        row = 1 if side == 0 else I
        if step == 0:
            src = x.at[pl.ds(half, half), row - 1, inside(c)]
        else:
            src = states[step % 2].at[pl.ds(1 + half, half), row, padded(c)]
        return pltpu.make_async_remote_copy(
            src_ref=src,
            dst_ref=relay.at[step, :, inside(c)],
            send_sem=relay_send.at[step, c],
            recv_sem=relay_recv.at[step, c],
            device_id={"lon": jnp.int32(0 if side == 0 else n_lon - 1)},
            device_id_type=MESH,
        )

    def from_relay(step, side, c):
        target = I + 1 if side == 0 else 0
        return pltpu.make_async_remote_copy(
            src_ref=relay.at[step, :, inside(c)],
            dst_ref=states[step % 2].at[pl.ds(1 + half, half), target, padded(c)],
            send_sem=pass_send.at[step, c],
            recv_sem=pass_recv.at[step, c],
            device_id={"lon": jnp.int32(n_lon // 2 - 1 if side == 0 else n_lon // 2)},
            device_id_type=MESH,
        )

    def relay_sides(step):
        return (0, 1) if step < STEPS - 1 else (1,)

    def lon_each(step, whole, split, arriving=False):
        for side in (0, 1):
            halved = me["lon"] == (n_lon // 2 if side == 0 else n_lon // 2 - 1)
            if (1 - side if arriving else side) in relay_sides(step):
                pl.when(jnp.logical_and(has("lon", side), jnp.logical_not(halved)))(
                    functools.partial(whole, side)
                )
                pl.when(halved)(functools.partial(split, side))
            else:
                pl.when(has("lon", side))(functools.partial(whole, side))

    def start_lon(step, c):
        def split(side):
            to_relay(step, side, c).start()
            lon_copy(step, side, c, count=half).start()

        lon_each(step, lambda side: lon_copy(step, side, c).start(), split)

    def sent_lon(step, c):
        def split(side):
            to_relay(step, side, c).wait_send()
            lon_copy(step, side, c, count=half).wait_send()

        lon_each(step, lambda side: lon_copy(step, side, c).wait_send(), split)

    def arrived_lon(step, c):
        def split(side):
            from_relay(step, 1 - side, c).wait_recv()
            lon_copy(step, side, c, True, half).wait_recv()

        lon_each(step, lambda side: lon_copy(step, side, c, True).wait_recv(), split, True)

    def relays(step, act):
        for side in relay_sides(step):
            pl.when(me["lon"] == (0 if side == 0 else n_lon - 1))(functools.partial(act, side))

    def forward(step, c):
        def act(side):
            to_relay(step, side, c).wait_recv()
            from_relay(step, side, c).start()

        relays(step, act)

    def lev_copy(step, side, arriving=False):
        slot = step % 2
        landing = side if arriving else 1 - side
        return pltpu.make_async_remote_copy(
            src_ref=lev_out.at[slot, side],
            dst_ref=lev_in.at[slot, landing],
            send_sem=lev_send.at[slot, side],
            recv_sem=lev_recv.at[slot, landing],
            device_id=beside("lev", side),
            device_id_type=MESH,
        )

    def send_chunk(step, c):
        start_lon(step, c)
        both("lat", lambda side: lat_copy(step, side, c).start())

    def sent_chunk(step, c):
        sent_lon(step, c)
        both("lat", lambda side: lat_copy(step, side, c).wait_send())

    def send_lev(step, side):
        state = states[step % 2]
        row = PAD if side == 0 else PAD + K - 1

        @pl.loop(1, J + 1)
        def _(p):
            lev_out[step % 2, side, p - 1] = state[p, 1 : I + 1, row : row + 1, :]

        lev_copy(step, side).start()

    def take_lev(step, side):
        state = states[step % 2]
        row = PAD - 1 if side == 0 else PAD + K
        lev_copy(step, side, True).wait_recv()

        @pl.loop(1, J + 1)
        def _(p):
            state[p, 1 : I + 1, row : row + 1, :] = lev_in[step % 2, side, p - 1]

    for c in range(FIRST):
        both("lat", lambda side: lat_copy(0, side, c).start())
    for which in range(3):
        for j in range(J):
            load(which, j).start()

    for n in range(ROUNDS):
        meet(rounds.at[n])
    for c in range(FIRST):
        start_lon(0, c)
    pl.loop(0, chunks)(lambda c: forward(0, c))
    pl.loop(FIRST, chunks)(lambda c: send_chunk(0, c))

    def clear(axis, side):
        for state in states:
            if axis == "lat":
                target = 0 if side == 0 else J + 1

                @pl.loop(1, I + 1)
                def _(i):
                    state[target, i, PAD : PAD + K, :] = jnp.zeros((K, M), jnp.float32)
            elif axis == "lon":
                target = 0 if side == 0 else I + 1
                for p in range(1, J + 1):
                    state[p, target, PAD : PAD + K, :] = jnp.zeros((K, M), jnp.float32)
            else:
                target = PAD - 1 if side == 0 else PAD + K

                @pl.loop(1, J + 1)
                def _(p):
                    state[p, 1 : I + 1, target : target + 1, :] = jnp.zeros(
                        (I, 1, M), jnp.float32
                    )

    for axis in ("lat", "lon", "lev"):
        for side in (0, 1):
            pl.when(jnp.logical_not(has(axis, side)))(functools.partial(clear, axis, side))

    for j in range(J):
        load(0, j).wait()
    both("lev", lambda side: send_lev(0, side))
    for j in range(J):
        load(1, j).wait()
        load(2, j).wait()

    def update(step, c, first, count):
        now, later = states[step % 2], states[(step + 1) % 2]
        last = step == STEPS - 1
        start = pl.multiple_of(PAD + c * CHUNK, CHUNK)
        here = pl.ds(start, CHUNK)
        inner = inside(c)

        def row(i, carry):
            past, mid, sums = carry
            coming = tuple(now[first + n, i + 1, here, :] for n in range(count))
            column = (now[first - 1, i, here, :],) + mid + (now[first + count, i, here, :],)
            out = []
            for n in range(count):
                p = first + n
                spread = (
                    (column[n] + column[n + 2])
                    + (past[n] + coming[n])
                    + (
                        now[p, i, pl.ds(start - 1, CHUNK), :]
                        + now[p, i, pl.ds(start + 1, CHUNK), :]
                    )
                    - 6.0 * mid[n]
                )
                new = (
                    mid[n]
                    + coef[p - 1, i - 1, inner, :] * spread
                    + source[p - 1, i - 1, inner, :]
                )
                if last:
                    end[p - 1, i - 1, inner, :] = new
                else:
                    later[p, i, here, :] = new
                out.append(new)
            if last:
                sums = tuple(total + new for total, new in zip(sums, out))
            return mid, coming, sums

        zero = jnp.zeros((CHUNK, M), jnp.float32)
        _, _, sums = lax.fori_loop(
            1,
            I + 1,
            row,
            (
                tuple(now[first + n, 0, here, :] for n in range(count)),
                tuple(now[first + n, 1, here, :] for n in range(count)),
                (zero,) * count if last else (),
            ),
            unroll=2 if count > 1 else 4,
        )
        return sums

    my_half = pl.ds(half * my_core, half)
    other_half = pl.ds(half * (1 - my_core), half)
    inner_plane = 1 + me["lat"]
    edge_plane = jnp.where(me["lat"] == 0, J, 1)
    partner = {"lon": me["lon"] + 1 - 2 * my_core}

    def mate_copy(c):
        return pltpu.make_async_remote_copy(
            src_ref=total.at[:, inside(c)],
            dst_ref=mate.at[:, inside(c)],
            send_sem=mate_send.at[c],
            recv_sem=mate_recv.at[c],
            device_id=partner,
            device_id_type=MESH,
        )

    def chip_copy(target, c, arriving=None):
        sender = my_chip if arriving is None else arriving
        return pltpu.make_async_remote_copy(
            src_ref=chip.at[:, inside(c)],
            dst_ref=chip_in.at[sender, :, inside(c)],
            send_sem=chip_send.at[target, c],
            recv_sem=chip_recv.at[sender, c],
            device_id={"lon": target * CORES + my_core},
            device_id_type=MESH,
        )

    def half_copy():
        return pltpu.make_async_remote_copy(
            src_ref=mine,
            dst_ref=theirs,
            send_sem=half_sem.at[0],
            recv_sem=half_sem.at[1],
            device_id=partner,
            device_id_type=MESH,
        )

    def edge_copy(target, arriving=None):
        sender = me["lon"] if arriving is None else arriving
        return pltpu.make_async_remote_copy(
            src_ref=edge,
            dst_ref=edge_in.at[sender],
            send_sem=edge_send.at[target],
            recv_sem=edge_recv.at[sender],
            device_id={"lon": jnp.int32(target)},
            device_id_type=MESH,
        )

    def later_chips(act):
        for other in range(1, n_chips):
            pl.when(other > my_chip)(functools.partial(act, other))

    def earlier_chips(act):
        for other in range(n_chips - 1):
            pl.when(other < my_chip)(functools.partial(act, other))

    def later_cores(act):
        for other in range(1, n_lon):
            pl.when(other > me["lon"])(functools.partial(act, other))

    def earlier_cores(act):
        for other in range(n_lon - 1):
            pl.when(other < me["lon"])(functools.partial(act, other))

    def share(c):
        mate_copy(c).wait()
        chip[:, inside(c), :] = total[my_half, inside(c), :] + mate[my_half, inside(c), :]
        later_chips(lambda other: chip_copy(other, c).start())

    def take_lon(step, c):
        arrived_lon(step, c)
        for side, end_chunk in ((0, 0), (1, chunks - 1)):
            pl.when(jnp.logical_and(c == end_chunk, has("lev", side)))(
                functools.partial(take_lev, step, side)
            )

    def send_lat(step, c):
        both("lat", lambda side: lat_copy(step, side, c).start())

    def take_lat(step, c):
        both("lat", lambda side: lat_copy(step, side, c, True).wait_recv())

    for step in range(STEPS - 1):
        if step > 0:
            forward(step, chunks - 1)

        @pl.loop(0, chunks)
        def _(c):
            if step > 0:
                sent_chunk(step - 1, c)
            take_lon(step, c)
            take_lat(step, c)
            update(step, c, 1, J)
            if step + 1 < STEPS - 1:
                pl.when(c > 0)(lambda: forward(step + 1, c - 1))
            if step < STEPS - 2:
                send_chunk(step + 1, c)
            else:
                start_lon(step + 1, c)
                pl.when(c < EARLY)(lambda: send_lat(step + 1, c))
            for side, end_chunk in ((0, 0), (1, chunks - 1)):

                def pass_on(side=side):
                    if step > 0:
                        lev_copy(step - 1, side).wait_send()
                    send_lev(step + 1, side)

                pl.when(jnp.logical_and(c == end_chunk, has("lev", side)))(pass_on)

    last = STEPS - 1
    for c in range(EARLY, AHEAD):
        send_lat(last, c)
    pl.loop(0, chunks)(lambda c: forward(last, c))
    for c in range(AHEAD, chunks):
        send_lat(last, c)

    @pl.loop(0, chunks)
    def _(c):
        sent_chunk(last - 1, c)
        take_lon(last, c)
        sums = update(last, c, inner_plane, J - 1)
        for n in range(J - 1):
            total[inner_plane - 1 + n, inside(c), :] = sums[n]

    def edge_step(c):
        take_lat(last, c)
        return update(last, c, edge_plane, 1)[0]

    tail = chunks - 1
    total[edge_plane - 1, inside(tail), :] = jnp.zeros((CHUNK, M), jnp.float32)
    mate_copy(tail).start()

    @pl.loop(0, tail)
    def _(c):
        total[edge_plane - 1, inside(c), :] = edge_step(c)
        mate_copy(c).start()
        pl.when(c > 0)(lambda: share(c - 1))

    share(tail)
    share(tail - 1)
    edge[...] = edge_step(tail)
    later_cores(lambda other: edge_copy(other).start())

    mine[...] = jnp.zeros(mine.shape, jnp.float32)

    def add_chip(other):
        for c in range(chunks):
            chip_copy(0, c, other).wait_recv()
        mine[...] += chip_in[other]

    earlier_chips(add_chip)
    half_copy().start()
    before[my_half] = mine[...]
    half_copy().wait()
    before[other_half] = theirs[...]

    @pl.when(my_core == 1)
    def _():
        before[...] += mate[...]

    def add_edge(other):
        edge_copy(0, other).wait_recv()
        before[edge_plane - 1, inside(tail), :] += edge_in[other]

    earlier_cores(add_edge)

    for step in (STEPS - 2, STEPS - 1):
        both("lev", lambda side: lev_copy(step, side).wait_send())
    for c in range(chunks):
        sent_chunk(STEPS - 1, c)
        later_chips(lambda other: chip_copy(other, c).wait_send())
    later_cores(lambda other: edge_copy(other).wait_send())
    for step in range(STEPS):
        pl.loop(0, chunks)(
            lambda c: relays(step, lambda side: from_relay(step, side, c).wait_send())
        )


def totals_kernel(scale, x, before, totals, end, sums, end_sem, sums_sem):
    J, I = x.shape[:2]

    def out(which, j):
        src, dst, sem = ((x, end, end_sem), (sums, totals, sums_sem))[which]
        return pltpu.make_async_copy(src.at[j], dst.at[j], sem.at[j])

    for j in range(J):
        out(0, j).start()

    @pl.loop(0, J)
    def _(j):
        def row(i, total):
            total = total + x[j, i]
            sums[j, i] = total * scale
            return total

        lax.fori_loop(0, I, row, before[j], unroll=4)
        out(1, j).start()

    for j in range(J):
        out(0, j).wait()
        out(1, j).wait()


def per_device(sizes, initial_state, scaled_diffusivity, scaled_forcing):
    J, I, K, M = initial_state.shape
    chunks = K // CHUNK
    n_lon = sizes["lon"]
    n_chips = n_lon // CORES
    half = J // CORES
    f32 = jnp.float32
    vmem = lambda *shape: pltpu.VMEM(shape, f32)
    sem = lambda *shape: pltpu.SemaphoreType.DMA(shape)
    hbm = pl.BlockSpec(memory_space=pltpu.HBM)
    local = pl.BlockSpec(memory_space=pltpu.VMEM)
    end, before = pl.pallas_call(
        functools.partial(steps_kernel, sizes),
        out_shape=(vmem(J, I, K, M), vmem(J, K, M)),
        in_specs=[hbm] * 3,
        out_specs=(local, local),
        scratch_shapes=[
            vmem(J + 2, I + 2, K + 2 * PAD, M),
            vmem(J + 2, I + 2, K + 2 * PAD, M),
            vmem(J, I, K, M),
            vmem(J, I, K, M),
            vmem(2, 2, J, I, 1, M),
            vmem(2, 2, J, I, 1, M),
            vmem(J, K, M),
            vmem(J, K, M),
            vmem(half, K, M),
            vmem(n_chips, half, K, M),
            vmem(half, K, M),
            vmem(half, K, M),
            vmem(CHUNK, M),
            vmem(n_lon, CHUNK, M),
            vmem(STEPS, half, K, M),
            sem(2, 2, chunks),
            sem(2, 2, chunks),
            sem(2, 2, chunks),
            sem(2, 2, chunks),
            sem(2, 2),
            sem(2, 2),
            sem(3, J),
            sem(chunks),
            sem(chunks),
            sem(n_chips, chunks),
            sem(n_chips, chunks),
            sem(2),
            sem(n_lon),
            sem(n_lon),
            sem(STEPS, chunks),
            sem(STEPS, chunks),
            sem(STEPS, chunks),
            sem(STEPS, chunks),
            pltpu.SemaphoreType.REGULAR((ROUNDS,)),
        ],
        compiler_params=pltpu.CompilerParams(
            collective_id=0, has_side_effects=True, vmem_limit_bytes=50 * 2**20
        ),
        name="steps",
    )(initial_state, scaled_diffusivity, scaled_forcing)

    return pl.pallas_call(
        functools.partial(totals_kernel, 1.0 / (I * n_lon)),
        out_shape=(jax.ShapeDtypeStruct((J, I, K, M), f32),) * 2,
        in_specs=[local, local],
        out_specs=(hbm, hbm),
        scratch_shapes=[vmem(J, I, K, M), sem(J), sem(J)],
        compiler_params=pltpu.CompilerParams(vmem_limit_bytes=20 * 2**20),
        name="totals",
    )(end, before)


def solution(mesh):
    spec = P("lat", "lon", "lev", None)
    return jax.shard_map(
        functools.partial(per_device, dict(mesh.shape)),
        mesh=mesh,
        in_specs=(spec,) * 3,
        out_specs=(spec,) * 2,
        check_vma=False,
    )
```

```python
import functools

import jax
import jax.numpy as jnp
from jax import lax
from jax.experimental import pallas as pl
from jax.experimental.pallas import tpu as pltpu
from jax.sharding import PartitionSpec as P

STEPS = 4
PAD = 8
CHUNK = 8
CORES = 2
EARLY = 2
AHEAD = 4
FIRST = 4
ROUNDS = 4
MESH = pl.DeviceIdType.MESH


def steps_kernel(
    sizes, x, d, f, end, before, even, odd, coef, source,
    lev_out, lev_in, total, mate, chip, chip_in, mine, theirs, edge, edge_in, relay,
    lat_send, lat_recv, lon_send, lon_recv, lev_send, lev_recv,
    load_sem, mate_send, mate_recv, chip_send, chip_recv, half_sem, edge_send, edge_recv,
    relay_send, relay_recv, pass_send, pass_recv, rounds,
):
    J, I, K, M = x.shape
    chunks = K // CHUNK
    states = (even, odd)
    me = {axis: lax.axis_index(axis) for axis in sizes}
    n_lon = sizes["lon"]
    n_chips = n_lon // CORES
    my_chip = me["lon"] // CORES
    my_core = me["lon"] % CORES
    half = J // CORES
    rows = pl.ds(1, I)
    levels = pl.ds(PAD, K)
    planes = pl.ds(1, J)

    def has(axis, side):
        return me[axis] > 0 if side == 0 else me[axis] < sizes[axis] - 1

    def beside(axis, side):
        return {axis: me[axis] - 1 if side == 0 else me[axis] + 1}

    def both(axis, act):
        if sizes[axis] > 1:
            for side in (0, 1):
                pl.when(has(axis, side))(functools.partial(act, side))

    def load(which, j):
        src, dst = (
            (x.at[j], even.at[j + 1, rows, levels]),
            (d.at[j], coef.at[j]),
            (f.at[j], source.at[j]),
        )[which]
        return pltpu.make_async_copy(src, dst, load_sem.at[which, j])

    barrier = pltpu.get_barrier_semaphore()
    lev_half, lon_half = sizes["lev"] // 2, n_lon // 2
    across, deep = me["lon"] // CORES % 2, me["lon"] // lon_half
    ring, lap = me["lev"] % lev_half, me["lev"] // lev_half
    side_x = 2 * across + me["lat"]
    side_z = 2 * lap + deep
    spot = lambda axis, index: {axis: index}
    near = (
        (jnp.bool_(True), spot("lat", 1 - me["lat"])),
        (jnp.bool_(True), spot("lon", me["lon"] + 1 - 2 * my_core)),
        (jnp.bool_(True), spot("lon", me["lon"] + lon_half - 2 * lon_half * deep)),
        (ring > 0, spot("lev", me["lev"] - 1)),
        (ring < lev_half - 1, spot("lev", me["lev"] + 1)),
        (
            jnp.logical_or(side_x == 1, side_x == 2),
            {"lat": 1 - me["lat"], "lon": me["lon"] + CORES - 2 * CORES * across},
        ),
        (
            jnp.logical_or(side_z == 1, side_z == 2),
            {
                "lon": me["lon"] + lon_half - 2 * lon_half * deep,
                "lev": me["lev"] + lev_half - 2 * lev_half * lap,
            },
        ),
    )
    peers = sum(there.astype(jnp.int32) for there, _ in near)

    def meet(semaphore):
        for there, target in near:
            pl.when(there)(
                lambda target=target: pl.semaphore_signal(
                    semaphore, inc=1, device_id=target, device_id_type=MESH
                )
            )
        pl.semaphore_wait(semaphore, peers)

    meet(barrier)

    def inside(c):
        return pl.ds(pl.multiple_of(c * CHUNK, CHUNK), CHUNK)

    def padded(c):
        return pl.ds(pl.multiple_of(PAD + c * CHUNK, CHUNK), CHUNK)

    def lat_copy(step, side, c, arriving=False):
        slot = step % 2
        state = states[slot]
        plane, target = (1, J + 1) if side == 0 else (J, 0)
        if arriving:
            target = 0 if side == 0 else J + 1
        if step == 0:
            src = x.at[plane - 1, :, inside(c)]
        else:
            src = state.at[plane, rows, padded(c)]
        return pltpu.make_async_remote_copy(
            src_ref=src,
            dst_ref=state.at[target, rows, padded(c)],
            send_sem=lat_send.at[slot, side, c],
            recv_sem=lat_recv.at[slot, side if arriving else 1 - side, c],
            device_id=beside("lat", side),
            device_id_type=MESH,
        )

    def lon_copy(step, side, c, arriving=False, count=J):
        slot = step % 2
        state = states[slot]
        row, target = (1, I + 1) if side == 0 else (I, 0)
        if arriving:
            target = 0 if side == 0 else I + 1
        if step == 0:
            src = x.at[pl.ds(0, count), row - 1, inside(c)]
        else:
            src = state.at[pl.ds(1, count), row, padded(c)]
        return pltpu.make_async_remote_copy(
            src_ref=src,
            dst_ref=state.at[pl.ds(1, count), target, padded(c)],
            send_sem=lon_send.at[slot, side, c],
            recv_sem=lon_recv.at[slot, side if arriving else 1 - side, c],
            device_id=beside("lon", side),
            device_id_type=MESH,
        )

    def to_relay(step, side, c):
        row = 1 if side == 0 else I
        if step == 0:
            src = x.at[pl.ds(half, half), row - 1, inside(c)]
        else:
            src = states[step % 2].at[pl.ds(1 + half, half), row, padded(c)]
        return pltpu.make_async_remote_copy(
            src_ref=src,
            dst_ref=relay.at[step, :, inside(c)],
            send_sem=relay_send.at[step, c],
            recv_sem=relay_recv.at[step, c],
            device_id={"lon": jnp.int32(0 if side == 0 else n_lon - 1)},
            device_id_type=MESH,
        )

    def from_relay(step, side, c):
        target = I + 1 if side == 0 else 0
        return pltpu.make_async_remote_copy(
            src_ref=relay.at[step, :, inside(c)],
            dst_ref=states[step % 2].at[pl.ds(1 + half, half), target, padded(c)],
            send_sem=pass_send.at[step, c],
            recv_sem=pass_recv.at[step, c],
            device_id={"lon": jnp.int32(n_lon // 2 - 1 if side == 0 else n_lon // 2)},
            device_id_type=MESH,
        )

    def relay_sides(step):
        return (0, 1) if step < STEPS - 1 else (1,)

    def lon_each(step, whole, split, arriving=False):
        for side in (0, 1):
            halved = me["lon"] == (n_lon // 2 if side == 0 else n_lon // 2 - 1)
            if (1 - side if arriving else side) in relay_sides(step):
                pl.when(jnp.logical_and(has("lon", side), jnp.logical_not(halved)))(
                    functools.partial(whole, side)
                )
                pl.when(halved)(functools.partial(split, side))
            else:
                pl.when(has("lon", side))(functools.partial(whole, side))

    def start_lon(step, c):
        def split(side):
            to_relay(step, side, c).start()
            lon_copy(step, side, c, count=half).start()

        lon_each(step, lambda side: lon_copy(step, side, c).start(), split)

    def sent_lon(step, c):
        def split(side):
            to_relay(step, side, c).wait_send()
            lon_copy(step, side, c, count=half).wait_send()

        lon_each(step, lambda side: lon_copy(step, side, c).wait_send(), split)

    def arrived_lon(step, c):
        def split(side):
            from_relay(step, 1 - side, c).wait_recv()
            lon_copy(step, side, c, True, half).wait_recv()

        lon_each(step, lambda side: lon_copy(step, side, c, True).wait_recv(), split, True)

    def relays(step, act):
        for side in relay_sides(step):
            pl.when(me["lon"] == (0 if side == 0 else n_lon - 1))(functools.partial(act, side))

    def forward(step, c):
        def act(side):
            to_relay(step, side, c).wait_recv()
            from_relay(step, side, c).start()

        relays(step, act)

    def lev_copy(step, side, arriving=False):
        slot = step % 2
        landing = side if arriving else 1 - side
        return pltpu.make_async_remote_copy(
            src_ref=lev_out.at[slot, side],
            dst_ref=lev_in.at[slot, landing],
            send_sem=lev_send.at[slot, side],
            recv_sem=lev_recv.at[slot, landing],
            device_id=beside("lev", side),
            device_id_type=MESH,
        )

    def send_chunk(step, c):
        start_lon(step, c)
        both("lat", lambda side: lat_copy(step, side, c).start())

    def sent_chunk(step, c):
        sent_lon(step, c)
        both("lat", lambda side: lat_copy(step, side, c).wait_send())

    def send_lev(step, side):
        state = states[step % 2]
        row = PAD if side == 0 else PAD + K - 1

        @pl.loop(1, J + 1)
        def _(p):
            lev_out[step % 2, side, p - 1] = state[p, 1 : I + 1, row : row + 1, :]

        lev_copy(step, side).start()

    def take_lev(step, side):
        state = states[step % 2]
        row = PAD - 1 if side == 0 else PAD + K
        lev_copy(step, side, True).wait_recv()

        @pl.loop(1, J + 1)
        def _(p):
            state[p, 1 : I + 1, row : row + 1, :] = lev_in[step % 2, side, p - 1]

    for c in range(FIRST):
        both("lat", lambda side: lat_copy(0, side, c).start())
    for which in range(3):
        for j in range(J):
            load(which, j).start()

    for n in range(ROUNDS - 1):
        meet(rounds.at[n])
    for c in range(FIRST):
        start_lon(0, c)
    pl.loop(0, chunks)(lambda c: forward(0, c))
    pl.loop(FIRST, chunks)(lambda c: send_chunk(0, c))
    meet(rounds.at[ROUNDS - 1])

    def clear(axis, side):
        for state in states:
            if axis == "lat":
                target = 0 if side == 0 else J + 1

                @pl.loop(1, I + 1)
                def _(i):
                    state[target, i, PAD : PAD + K, :] = jnp.zeros((K, M), jnp.float32)
            elif axis == "lon":
                target = 0 if side == 0 else I + 1
                for p in range(1, J + 1):
                    state[p, target, PAD : PAD + K, :] = jnp.zeros((K, M), jnp.float32)
            else:
                target = PAD - 1 if side == 0 else PAD + K

                @pl.loop(1, J + 1)
                def _(p):
                    state[p, 1 : I + 1, target : target + 1, :] = jnp.zeros(
                        (I, 1, M), jnp.float32
                    )

    for axis in ("lat", "lon", "lev"):
        for side in (0, 1):
            pl.when(jnp.logical_not(has(axis, side)))(functools.partial(clear, axis, side))

    for j in range(J):
        load(0, j).wait()
    both("lev", lambda side: send_lev(0, side))
    for j in range(J):
        load(1, j).wait()
        load(2, j).wait()

    def update(step, c, first, count):
        now, later = states[step % 2], states[(step + 1) % 2]
        last = step == STEPS - 1
        start = pl.multiple_of(PAD + c * CHUNK, CHUNK)
        here = pl.ds(start, CHUNK)
        inner = inside(c)

        def row(i, carry):
            past, mid, sums = carry
            coming = tuple(now[first + n, i + 1, here, :] for n in range(count))
            column = (now[first - 1, i, here, :],) + mid + (now[first + count, i, here, :],)
            out = []
            for n in range(count):
                p = first + n
                spread = (
                    (column[n] + column[n + 2])
                    + (past[n] + coming[n])
                    + (
                        now[p, i, pl.ds(start - 1, CHUNK), :]
                        + now[p, i, pl.ds(start + 1, CHUNK), :]
                    )
                    - 6.0 * mid[n]
                )
                new = (
                    mid[n]
                    + coef[p - 1, i - 1, inner, :] * spread
                    + source[p - 1, i - 1, inner, :]
                )
                if last:
                    end[p - 1, i - 1, inner, :] = new
                else:
                    later[p, i, here, :] = new
                out.append(new)
            if last:
                sums = tuple(total + new for total, new in zip(sums, out))
            return mid, coming, sums

        zero = jnp.zeros((CHUNK, M), jnp.float32)
        _, _, sums = lax.fori_loop(
            1,
            I + 1,
            row,
            (
                tuple(now[first + n, 0, here, :] for n in range(count)),
                tuple(now[first + n, 1, here, :] for n in range(count)),
                (zero,) * count if last else (),
            ),
            unroll=2 if count > 1 else 4,
        )
        return sums

    my_half = pl.ds(half * my_core, half)
    other_half = pl.ds(half * (1 - my_core), half)
    inner_plane = 1 + me["lat"]
    edge_plane = jnp.where(me["lat"] == 0, J, 1)
    partner = {"lon": me["lon"] + 1 - 2 * my_core}

    def mate_copy(c):
        return pltpu.make_async_remote_copy(
            src_ref=total.at[:, inside(c)],
            dst_ref=mate.at[:, inside(c)],
            send_sem=mate_send.at[c],
            recv_sem=mate_recv.at[c],
            device_id=partner,
            device_id_type=MESH,
        )

    def chip_copy(target, c, arriving=None):
        sender = my_chip if arriving is None else arriving
        return pltpu.make_async_remote_copy(
            src_ref=chip.at[:, inside(c)],
            dst_ref=chip_in.at[sender, :, inside(c)],
            send_sem=chip_send.at[target, c],
            recv_sem=chip_recv.at[sender, c],
            device_id={"lon": target * CORES + my_core},
            device_id_type=MESH,
        )

    def half_copy():
        return pltpu.make_async_remote_copy(
            src_ref=mine,
            dst_ref=theirs,
            send_sem=half_sem.at[0],
            recv_sem=half_sem.at[1],
            device_id=partner,
            device_id_type=MESH,
        )

    def edge_copy(target, arriving=None):
        sender = me["lon"] if arriving is None else arriving
        return pltpu.make_async_remote_copy(
            src_ref=edge,
            dst_ref=edge_in.at[sender],
            send_sem=edge_send.at[target],
            recv_sem=edge_recv.at[sender],
            device_id={"lon": jnp.int32(target)},
            device_id_type=MESH,
        )

    def later_chips(act):
        for other in range(1, n_chips):
            pl.when(other > my_chip)(functools.partial(act, other))

    def earlier_chips(act):
        for other in range(n_chips - 1):
            pl.when(other < my_chip)(functools.partial(act, other))

    def later_cores(act):
        for other in range(1, n_lon):
            pl.when(other > me["lon"])(functools.partial(act, other))

    def earlier_cores(act):
        for other in range(n_lon - 1):
            pl.when(other < me["lon"])(functools.partial(act, other))

    def share(c):
        mate_copy(c).wait()
        chip[:, inside(c), :] = total[my_half, inside(c), :] + mate[my_half, inside(c), :]
        later_chips(lambda other: chip_copy(other, c).start())

    def take_lon(step, c):
        arrived_lon(step, c)
        for side, end_chunk in ((0, 0), (1, chunks - 1)):
            pl.when(jnp.logical_and(c == end_chunk, has("lev", side)))(
                functools.partial(take_lev, step, side)
            )

    def send_lat(step, c):
        both("lat", lambda side: lat_copy(step, side, c).start())

    def take_lat(step, c):
        both("lat", lambda side: lat_copy(step, side, c, True).wait_recv())

    for step in range(STEPS - 1):
        if step > 0:
            forward(step, chunks - 1)

        @pl.loop(0, chunks)
        def _(c):
            if step > 0:
                sent_chunk(step - 1, c)
            take_lon(step, c)
            take_lat(step, c)
            update(step, c, 1, J)
            if step + 1 < STEPS - 1:
                pl.when(c > 0)(lambda: forward(step + 1, c - 1))
            if step < STEPS - 2:
                send_chunk(step + 1, c)
            else:
                start_lon(step + 1, c)
                pl.when(c < EARLY)(lambda: send_lat(step + 1, c))
            for side, end_chunk in ((0, 0), (1, chunks - 1)):

                def pass_on(side=side):
                    if step > 0:
                        lev_copy(step - 1, side).wait_send()
                    send_lev(step + 1, side)

                pl.when(jnp.logical_and(c == end_chunk, has("lev", side)))(pass_on)

    last = STEPS - 1
    for c in range(EARLY, AHEAD):
        send_lat(last, c)
    pl.loop(0, chunks)(lambda c: forward(last, c))
    for c in range(AHEAD, chunks):
        send_lat(last, c)

    @pl.loop(0, chunks)
    def _(c):
        sent_chunk(last - 1, c)
        take_lon(last, c)
        sums = update(last, c, inner_plane, J - 1)
        for n in range(J - 1):
            total[inner_plane - 1 + n, inside(c), :] = sums[n]

    def edge_step(c):
        take_lat(last, c)
        return update(last, c, edge_plane, 1)[0]

    tail = chunks - 1
    total[edge_plane - 1, inside(tail), :] = jnp.zeros((CHUNK, M), jnp.float32)
    mate_copy(tail).start()

    @pl.loop(0, tail)
    def _(c):
        total[edge_plane - 1, inside(c), :] = edge_step(c)
        mate_copy(c).start()
        pl.when(c > 0)(lambda: share(c - 1))

    share(tail)
    share(tail - 1)
    edge[...] = edge_step(tail)
    later_cores(lambda other: edge_copy(other).start())

    mine[...] = jnp.zeros(mine.shape, jnp.float32)

    def add_chip(other):
        for c in range(chunks):
            chip_copy(0, c, other).wait_recv()
        mine[...] += chip_in[other]

    earlier_chips(add_chip)
    half_copy().start()
    before[my_half] = mine[...]
    half_copy().wait()
    before[other_half] = theirs[...]

    @pl.when(my_core == 1)
    def _():
        before[...] += mate[...]

    def add_edge(other):
        edge_copy(0, other).wait_recv()
        before[edge_plane - 1, inside(tail), :] += edge_in[other]

    earlier_cores(add_edge)

    for step in (STEPS - 2, STEPS - 1):
        both("lev", lambda side: lev_copy(step, side).wait_send())
    for c in range(chunks):
        sent_chunk(STEPS - 1, c)
        later_chips(lambda other: chip_copy(other, c).wait_send())
    later_cores(lambda other: edge_copy(other).wait_send())
    for step in range(STEPS):
        pl.loop(0, chunks)(
            lambda c: relays(step, lambda side: from_relay(step, side, c).wait_send())
        )


def totals_kernel(scale, x, before, totals, end, sums, end_sem, sums_sem):
    J, I = x.shape[:2]

    def out(which, j):
        src, dst, sem = ((x, end, end_sem), (sums, totals, sums_sem))[which]
        return pltpu.make_async_copy(src.at[j], dst.at[j], sem.at[j])

    for j in range(J):
        out(0, j).start()

    @pl.loop(0, J)
    def _(j):
        def row(i, total):
            total = total + x[j, i]
            sums[j, i] = total * scale
            return total

        lax.fori_loop(0, I, row, before[j], unroll=4)
        out(1, j).start()

    for j in range(J):
        out(0, j).wait()
        out(1, j).wait()


def per_device(sizes, initial_state, scaled_diffusivity, scaled_forcing):
    J, I, K, M = initial_state.shape
    chunks = K // CHUNK
    n_lon = sizes["lon"]
    n_chips = n_lon // CORES
    half = J // CORES
    f32 = jnp.float32
    vmem = lambda *shape: pltpu.VMEM(shape, f32)
    sem = lambda *shape: pltpu.SemaphoreType.DMA(shape)
    hbm = pl.BlockSpec(memory_space=pltpu.HBM)
    local = pl.BlockSpec(memory_space=pltpu.VMEM)
    end, before = pl.pallas_call(
        functools.partial(steps_kernel, sizes),
        out_shape=(vmem(J, I, K, M), vmem(J, K, M)),
        in_specs=[hbm] * 3,
        out_specs=(local, local),
        scratch_shapes=[
            vmem(J + 2, I + 2, K + 2 * PAD, M),
            vmem(J + 2, I + 2, K + 2 * PAD, M),
            vmem(J, I, K, M),
            vmem(J, I, K, M),
            vmem(2, 2, J, I, 1, M),
            vmem(2, 2, J, I, 1, M),
            vmem(J, K, M),
            vmem(J, K, M),
            vmem(half, K, M),
            vmem(n_chips, half, K, M),
            vmem(half, K, M),
            vmem(half, K, M),
            vmem(CHUNK, M),
            vmem(n_lon, CHUNK, M),
            vmem(STEPS, half, K, M),
            sem(2, 2, chunks),
            sem(2, 2, chunks),
            sem(2, 2, chunks),
            sem(2, 2, chunks),
            sem(2, 2),
            sem(2, 2),
            sem(3, J),
            sem(chunks),
            sem(chunks),
            sem(n_chips, chunks),
            sem(n_chips, chunks),
            sem(2),
            sem(n_lon),
            sem(n_lon),
            sem(STEPS, chunks),
            sem(STEPS, chunks),
            sem(STEPS, chunks),
            sem(STEPS, chunks),
            pltpu.SemaphoreType.REGULAR((ROUNDS,)),
        ],
        compiler_params=pltpu.CompilerParams(
            collective_id=0, has_side_effects=True, vmem_limit_bytes=50 * 2**20
        ),
        name="steps",
    )(initial_state, scaled_diffusivity, scaled_forcing)

    return pl.pallas_call(
        functools.partial(totals_kernel, 1.0 / (I * n_lon)),
        out_shape=(jax.ShapeDtypeStruct((J, I, K, M), f32),) * 2,
        in_specs=[local, local],
        out_specs=(hbm, hbm),
        scratch_shapes=[vmem(J, I, K, M), sem(J), sem(J)],
        compiler_params=pltpu.CompilerParams(vmem_limit_bytes=20 * 2**20),
        name="totals",
    )(end, before)


def solution(mesh):
    spec = P("lat", "lon", "lev", None)
    return jax.shard_map(
        functools.partial(per_device, dict(mesh.shape)),
        mesh=mesh,
        in_specs=(spec,) * 3,
        out_specs=(spec,) * 2,
        check_vma=False,
    )
```
